32 devices in a mesh: groups: 2 (over x), tile: 8 (over z, y), link: 2 (over core).
Axes of the slice: x: 2, y: 2, z: 4, core: 2. Of those that a mesh axis runs over, the one named last changes fastest.
Arguments:
- points: float32 [9, 30, 2048], P(None, None, ('groups', 'tile')), parts along dimension 2, may hold values from -12 to 12
- potentials: float32 [9, 2048], P(None, ('groups', 'tile')), parts along dimension 1, may hold values from -6 to 124
Outputs:
- residual: float32 [8, 2048], P('link', ('groups', 'tile')), parts along dimension 1
The draws below stay inside these ranges and needn't reach their ends.
There are 2 independent parts, one for each index of `groups`. The reference program is written for one: setup_inputs(seed, part) draws one part's arguments, and reference() takes and returns one part's arrays. A program takes and returns all parts, laid end to end along the dimension named above; each array names one. Nothing has to cross between parts.
All inputs are finite; a program needn't handle non-finite values.
Results may differ from the reference program's by a relative error of at most 0.0003.
Values sent between devices are 32-bit elements; how exact they have to be, the bound alone decides.
A program may use at most 128 MiB of HBM per device.

```python
import math
import jax
import jax.numpy as jnp
from jax import lax

PCS = 30
LINKS = 8
TIMES = 9
CELLS = 1024


def draw_points(key, part):
    key_drift, key_base = jax.random.split(jax.random.fold_in(key, 11), 2)
    drift = jax.random.normal(key_drift, (TIMES, PCS, 1), jnp.float32) * 0.15
    values = jax.random.normal(key_base, (TIMES, PCS, CELLS), jnp.float32) * 0.5 + drift
    return jnp.clip(values, -12.0, 12.0).astype(jnp.float32)


def draw_potentials(key, part):
    key_base = jax.random.fold_in(jax.random.fold_in(key, 23), 0)
    values = jnp.clip(jax.random.normal(key_base, (TIMES, CELLS), jnp.float32) * 1.5, -5.0, 5.0)
    return values.astype(jnp.float32)


def setup_inputs(seed: int = 0, part: int = 0) -> dict:
    seeds = jax.random.split(jax.random.key(seed), 3)
    own_keys = jax.random.split(jax.random.fold_in(seeds[2], part), 3)
    return {
        "points": draw_points(jax.random.fold_in(jax.random.fold_in(seeds[2], part), 71), part),
        "potentials": draw_potentials(jax.random.fold_in(jax.random.fold_in(seeds[2], part), 71), part),
    }


EPSILON = 0.5


def pair_scores(source_pts, target_pts, source_msg):
    source_sq = jnp.sum(source_pts * source_pts, axis=0)
    target_sq = jnp.sum(target_pts * target_pts, axis=0)
    inner_prod = lax.dot_general(source_pts, target_pts, (((0,), (0,)), ((), ())), precision=lax.Precision.HIGHEST, preferred_element_type=jnp.float32)
    pair_cost = source_sq[:, None] + target_sq[None, :] - 2.0 * inner_prod
    return source_msg[:, None] - pair_cost / EPSILON


def link_message(source_pts, target_pts, source_msg, target_pot):
    width = math.gcd(target_pts.shape[1], 512)
    blocks = target_pts.reshape(target_pts.shape[0], -1, width).transpose(1, 0, 2)

    def one_block(block):
        scores = pair_scores(source_pts, block, source_msg)
        peak = jnp.max(scores, axis=0)
        return peak + jnp.log(jnp.sum(jnp.exp(scores - peak[None, :]), axis=0))

    return target_pot + lax.map(one_block, blocks).reshape(-1)


def reference(points, potentials):
    forward_msgs = [potentials[0]]
    for link_step in range(LINKS):
        forward_msgs.append(link_message(points[link_step], points[link_step + 1], forward_msgs[-1], potentials[link_step + 1]))
    backward_msgs = [potentials[LINKS]]
    for link_step in range(LINKS - 1, -1, -1):
        backward_msgs.insert(0, link_message(points[link_step + 1], points[link_step], backward_msgs[0], potentials[link_step]))
    combined = jnp.stack(forward_msgs) + jnp.stack(backward_msgs) - potentials
    last_row = combined[LINKS]
    peak = jnp.max(last_row)
    log_total = peak + jnp.log(jnp.sum(jnp.exp(last_row - peak)))
    return -math.log(CELLS) - (combined[1:] - log_total)
```

```python
import functools
import math

import jax
import jax.numpy as jnp
from jax import lax
from jax.experimental import pallas as pl
from jax.experimental.pallas import tpu as pltpu
from jax.sharding import PartitionSpec as P

EPSILON = 0.5
LOG2E = math.log2(math.e)
SCALE = 2.0 / EPSILON * LOG2E
STRIP = 1024
ROWS = 8
BLOCK = 64
WAYS = 2
DIRECT = 0


def pieces(value):
    high = value.astype(jnp.bfloat16)
    rest = value - high.astype(jnp.float32)
    middle = rest.astype(jnp.bfloat16)
    low = (rest - middle.astype(jnp.float32)).astype(jnp.bfloat16)
    return high, middle, low


def padded(points, extra):
    pad = 32 - points.shape[0]
    row = lax.broadcasted_iota(jnp.int32, (pad, points.shape[1]), 0)
    tail = jnp.where(row == 0, 0.0 if extra is None else extra, 0.0)
    return jnp.concatenate([points, tail], axis=0)


class Chain:
    def __init__(self, links, tiles, pts, pot, right, left, score, alpha, const, rest, col, own, tops, me, time):
        self.links, self.tiles = links, tiles
        self.pts, self.pot = pts, pot
        self.right, self.left, self.score = right, left, score
        self.alpha, self.const, self.rest = alpha, const, rest
        self.col, self.own, self.tops = col, own, tops
        self.me, self.time = me, time

    def constants(self, k, r):
        t = self.time(k)
        x = self.pts[t, r]
        lanes = pl.ds(pl.multiple_of(r * 128, 128), 128)
        square = jnp.sum(x * x, axis=0, keepdims=True)
        pot = self.pot[r, pl.ds(t, 1), :]
        self.const[t, :, lanes] = (pot - (2.0 / EPSILON) * square) * LOG2E
        if k == 0:
            self.alpha[t, :, lanes] = (pot - square / EPSILON) * LOG2E
        if k == self.links:
            self.rest[:, lanes] = square * (LOG2E / EPSILON)

    def prep_even(self, k, link, r):
        x = self.pts[self.time(k), r]
        one = jnp.full((1, 128), 1.0 if link % 2 == 0 else 0.0, jnp.float32)
        h, m, l = pieces(padded(x, one))
        zero = jnp.zeros_like(h)
        lanes = pl.ds(pl.multiple_of(r * 128, 128), 128)
        self.right[link % 2][:, lanes] = jnp.concatenate([h, h, h, m, l, m, zero, zero], axis=0)

    def prep_odd(self, k, r):
        t = self.time(k)
        lanes = pl.ds(pl.multiple_of(r * 128, 128), 128)
        x = padded(self.pts[t, r] * SCALE, self.const[t, :, lanes])
        h, m, l = pieces(x)
        block = jnp.concatenate([h, m, l, h], axis=0)
        block = block.T
        slot = (k // 2) % 2
        self.left[slot][lanes, 0:128] = block
        self.left[slot][lanes, 128:256] = block

    def prep(self, link, r):
        if link % 2 == 0:
            if link == 0:
                self.constants(0, r)
                self.prep_even(0, link, r)
            else:
                self.prep_even(link, link, r)
            self.constants(link + 1, r)
            self.prep_odd(link + 1, r)
        else:
            self.constants(link + 1, r)
            self.prep_even(link + 1, link, r)

    def product(self, link, i):
        lanes = pl.ds(pl.multiple_of(i * STRIP, STRIP), STRIP)
        slot = (link // 2) % 2
        self.score[link % 2][:, lanes] = jnp.dot(
            self.left[slot][...], self.right[link % 2][:, lanes], preferred_element_type=jnp.float32
        )

    def reduce_lanes(self, i):
        for j in range(STRIP // ROWS):
            rows = pl.ds(pl.multiple_of(i * STRIP + j * ROWS, ROWS), ROWS)
            top = self.tops[rows, :]
            peak = jnp.max(top, axis=1, keepdims=True)
            total = jnp.sum(self.col[rows, :] * jnp.exp2(top - peak), axis=1, keepdims=True)
            out = peak + jnp.log(total) * LOG2E
            self.col[rows, :] = jnp.broadcast_to(out, (ROWS, 128))

    def message(self, link, i):
        t = self.time(link)
        after = self.time(link + 1)
        if link % 2 == 0:
            source = self.alpha[t]
            rows = pl.ds(pl.multiple_of(i * STRIP, STRIP), STRIP)
            dots = jnp.dot(self.left[(link // 2) % 2][rows, :], self.right[0][...], preferred_element_type=jnp.float32)
            tiles = [slice(j * 128, (j + 1) * 128) for j in range(self.tiles)]
            for j in range(STRIP // ROWS):
                rows = pl.ds(pl.multiple_of(i * STRIP + j * ROWS, ROWS), ROWS)
                s = [dots[j * ROWS:(j + 1) * ROWS, c] + source[:, c] for c in tiles]
                top = functools.reduce(jnp.maximum, s)
                self.tops[rows, :] = top
                self.col[rows, :] = functools.reduce(jnp.add, [jnp.exp2(a - top) for a in s])
        else:
            lanes = pl.ds(pl.multiple_of(i * STRIP, STRIP), STRIP)
            cells = self.col.shape[0]
            step = BLOCK
            peak = total = None
            dots = jnp.dot(self.left[(link // 2) % 2][...], self.right[1][:, lanes], preferred_element_type=jnp.float32)
            for j in range(cells // step):
                rows = slice(j * step, (j + 1) * step)
                source = self.col[rows, :]
                s = dots[rows, :] + jnp.concatenate([source] * (STRIP // 128), axis=1)
                s = s.reshape(step // 8, 8, STRIP)
                top = jnp.max(s, axis=0)
                if peak is None:
                    peak = top
                    total = jnp.sum(jnp.exp2(s - peak[None]), axis=0)
                else:
                    new = jnp.maximum(peak, top)
                    total = total * jnp.exp2(peak - new) + jnp.sum(jnp.exp2(s - new[None]), axis=0)
                    peak = new
            top = jnp.max(peak, axis=0, keepdims=True)
            total = jnp.sum(total * jnp.exp2(peak - top), axis=0, keepdims=True)
            self.alpha[after, :, lanes] = self.const[after, :, lanes] + top + jnp.log(total) * LOG2E

    def keep(self, k):
        t = self.time(k)
        mine = pl.ds(pl.multiple_of(self.me * 128, 128), 128)
        if k % 2 == 0:
            self.own[t] = self.alpha[t, :, mine]
        else:
            block = self.col[mine, :]
            eye = lax.broadcasted_iota(jnp.int32, (128, 128), 0) == lax.broadcasted_iota(
                jnp.int32, (128, 128), 1
            )
            self.own[t] = jnp.sum(jnp.where(eye, block, 0.0), axis=0, keepdims=True)

    def log_total(self):
        phi = self.alpha[self.time(self.links)] + self.rest[...]
        peak = jnp.max(phi, axis=1, keepdims=True)
        return peak + jnp.log(jnp.sum(jnp.exp2(phi - peak), axis=1, keepdims=True)) * LOG2E

    def loop(self, count, body):
        def turn(i, carry):
            body(i)
            return carry

        lax.fori_loop(0, count, turn, 0)

    def run(self, ready, done):
        turns = self.tiles * 128 // STRIP
        share = self.tiles // turns
        ready(1)
        self.loop(self.tiles, lambda r: self.prep(0, r))
        ready(2)
        self.loop(self.tiles, lambda r: self.prep(1, r))
        for link in range(self.links):
            if link + 3 <= self.links:
                ready(link + 3)

            def body(i, link=link):
                self.message(link, i)
                if link + 2 < self.links:
                    for j in range(share):
                        self.prep(link + 2, i * share + j)

            self.loop(turns, body)
            if link % 2 == 0:
                self.loop(turns, self.reduce_lanes)
            self.keep(link + 1)
            done(link + 1)


def chain_kernel(links, tiles, pts, pot, out, *scratch):
    held, pots, *pairs = scratch[:8]
    right, left, score = pairs[0:2], pairs[2:4], pairs[4:6]
    alpha, const, rest, col, own, other = scratch[8:14]
    line_send, line_recv, pair_send, pair_recv, core_send, core_recv, end_send, end_recv = scratch[14:22]
    fill, tops = scratch[22:]
    me = lax.axis_index("tile")
    way = lax.axis_index("link")
    line = tiles // 2
    at, side = me // 2, me % 2
    half = links // 2
    chunks = [(k, 1) for k in range(half + 1)]
    time = lambda k: k + way * (links - 2 * k)
    first = lambda k, count: k + way * (links - 2 * k - count + 1)
    slot = lambda z, y: 2 * z + y
    ahead = lambda d: slot(lax.rem(at + d, line), side)
    behind = lambda d: lax.rem(at + line - d, line)
    chain = Chain(
        links, tiles, held, pots, right, left, score, alpha, const, rest, col, own, tops, me, time
    )

    early = pl.ds(way * half, half + 1)
    mine = [
        pltpu.make_async_copy(pot, pots.at[me], fill.at[0]),
        pltpu.make_async_copy(pts.at[early], held.at[early, me], fill.at[1]),
    ]
    for copy in mine:
        copy.start()

    barrier = pltpu.get_barrier_semaphore()
    peers = [{"tile": ahead(d)} for d in range(1, line)]
    peers += [{"tile": slot(at, 1 - side)}, {"link": 1 - way}]
    for peer in peers:
        pl.semaphore_signal(barrier, inc=1, device_id=peer)
    pl.semaphore_wait(barrier, len(peers))

    def views(c, origin, source_own):
        if c == 0:
            return (pot if source_own else pots.at[origin]), pots.at[origin]
        k, count = chunks[c - 1]
        span = pl.ds(first(k, count), count)
        return (pts.at[span] if source_own else held.at[span, origin]), held.at[span, origin]

    def remote(c, origin, source_own, send, recv, d, device):
        src, dst = views(c, origin, source_own)
        return pltpu.make_async_remote_copy(
            src_ref=src,
            dst_ref=dst,
            send_sem=send.at[c, d],
            recv_sem=recv.at[c, d],
            device_id=device,
        )

    partner = {"tile": slot(at, 1 - side)}
    sent = []

    def to_line(c, d):
        copy = remote(c, me, True, line_send, line_recv, d, {"tile": ahead(d)})
        copy.start()
        sent.append(copy)

    def to_cross(c, d):
        device = {"tile": slot(lax.rem(at + d, line), 1 - side)}
        copy = remote(c, me, True, pair_send, pair_recv, d, device)
        copy.start()
        sent.append(copy)

    def to_pair(c, d):
        origin = slot(behind(d), side)
        copy = remote(c, origin, d == 0, pair_send, pair_recv, d, partner)
        copy.start()
        sent.append(copy)

    def forward(c):
        for d in range(1, line):
            origin = slot(behind(d), side)
            remote(c, origin, False, line_send, line_recv, d, partner).wait_recv()
            if c >= DIRECT:
                to_pair(c, d)

    def arrive(c):
        for d in range(line):
            origin = slot(behind(d), 1 - side)
            remote(c, origin, False, pair_send, pair_recv, d, partner).wait_recv()

    def across(k):
        t = time(k)
        copy = pltpu.make_async_remote_copy(
            src_ref=held.at[t],
            dst_ref=held.at[t],
            send_sem=core_send.at[k],
            recv_sem=core_recv.at[k],
            device_id={"link": 1 - way},
        )
        copy.start()
        sent.append(copy)

    def from_core(k):
        t = time(links - k)
        pltpu.make_async_remote_copy(
            src_ref=held.at[t],
            dst_ref=held.at[t],
            send_sem=core_send.at[k],
            recv_sem=core_recv.at[k],
            device_id={"link": 1 - way},
        ).wait_recv()

    def rows(which):
        return pl.ds(first(half, half), half) if which == 0 else pl.ds(time(links), 1)

    def ends(which, span):
        return pltpu.make_async_remote_copy(
            src_ref=own.at[span],
            dst_ref=other.at[span],
            send_sem=end_send.at[which],
            recv_sem=end_recv.at[which],
            device_id={"link": 1 - way},
        )

    for c in range(len(chunks) + 1):
        for d in range(line - 1, 0, -1):
            if c < DIRECT:
                to_cross(c, d)
            to_line(c, d)
        to_pair(c, 0)

    def ready(k):
        if k == 1:
            for copy in mine:
                copy.wait()
            for c in range(4):
                forward(c)
            for c in range(3):
                arrive(c)
            across(1)
            across(0)
        elif k <= half:
            if k < half:
                forward(k + 2)
            arrive(k + 1)
            if k < half:
                across(k)
        else:
            from_core(links - k)

    def done(k):
        if k == links - 1:
            copy = ends(0, rows(0))
            copy.start()
            sent.append(copy)
        if k == links:
            copy = ends(1, rows(1))
            copy.start()
            sent.append(copy)

    chain.run(ready, done)
    chain.keep(0)
    total = chain.log_total()
    ends(0, rows_other(0, links, half, way)).wait_recv()
    ends(1, rows_other(1, links, half, way)).wait_recv()
    lanes = pl.ds(pl.multiple_of(me * 128, 128), 128)
    keep = -math.log(tiles * 128)
    for j in range(half):
        t = 1 + way * half + j
        combined = own[t] + other[t] - const[t, :, lanes]
        out[pl.ds(j, 1), :] = keep - (combined - total) / LOG2E
    for copy in sent:
        copy.wait_send()


def rows_other(which, links, half, way):
    back = 1 - way
    if which == 0:
        return pl.ds(half + back * (1 - half), half)
    return pl.ds(links - back * links, 1)


def local_fast(points, potentials):
    times, pcs, cell_dev = points.shape
    links = times - 1
    tiles = lax.axis_size("tile")
    cells = tiles * cell_dev
    vmem = pl.BlockSpec(memory_space=pltpu.VMEM)
    hbm = pl.BlockSpec(memory_space=pltpu.HBM)
    dma = pltpu.SemaphoreType.DMA
    phases = links // 2 + 2
    line = tiles // 2
    return pl.pallas_call(
        functools.partial(chain_kernel, links, tiles),
        out_shape=jax.ShapeDtypeStruct((links // 2, 128), jnp.float32),
        in_specs=[hbm] * 2,
        out_specs=vmem,
        scratch_shapes=[
            pltpu.VMEM((times, tiles, pcs, 128), jnp.float32),
            pltpu.VMEM((tiles, times, 128), jnp.float32),
            pltpu.VMEM((256, cells), jnp.bfloat16),
            pltpu.VMEM((256, cells), jnp.bfloat16),
            pltpu.VMEM((cells, 256), jnp.bfloat16),
            pltpu.VMEM((cells, 256), jnp.bfloat16),
            pltpu.VMEM((cells, cells), jnp.float32),
            pltpu.VMEM((cells, cells), jnp.float32),
            pltpu.VMEM((times, 1, cells), jnp.float32),
            pltpu.VMEM((times, 1, cells), jnp.float32),
            pltpu.VMEM((1, cells), jnp.float32),
            pltpu.VMEM((cells, 128), jnp.float32),
            pltpu.VMEM((times, 1, 128), jnp.float32),
            pltpu.VMEM((times, 1, 128), jnp.float32),
            dma((phases, line)),
            dma((phases, line)),
            dma((phases, line)),
            dma((phases, line)),
            dma((links // 2,)),
            dma((links // 2,)),
            dma((2,)),
            dma((2,)),
            dma((2,)),
            pltpu.VMEM((cells, 128), jnp.float32),
        ],
        compiler_params=pltpu.CompilerParams(
            vmem_limit_bytes=66900000, collective_id=0, has_side_effects=True
        ),
    )(points, potentials)


def passed_along(block, axis, distance):
    devices = range(lax.axis_size(axis))
    route = [(i - distance, i) for i in devices if i - distance in devices]
    return lax.ppermute(block, axis, route)


def joined(part, axis, combine):
    gathered = jax.tree.map(lambda a: lax.all_gather(a, axis), part)

    def take(source):
        return jax.tree.map(lambda a: lax.dynamic_index_in_dim(a, source, 0, False), gathered)

    return lax.fori_loop(
        1, lax.axis_size(axis), lambda source, state: combine(state, take(source)), take(0)
    )


def pair_scores(source_pts, target_pts, source_msg):
    source_sq = jnp.sum(source_pts * source_pts, axis=0)
    target_sq = jnp.sum(target_pts * target_pts, axis=0)
    inner_prod = lax.dot_general(
        source_pts,
        target_pts,
        (((0,), (0,)), ((), ())),
        precision=lax.Precision.HIGHEST,
        preferred_element_type=jnp.float32,
    )
    pair_cost = source_sq[:, None] + target_sq[None, :] - 2.0 * inner_prod
    return source_msg[:, None] - pair_cost / EPSILON


def combine_lse(left_pair, right_pair):
    peak = jnp.maximum(left_pair[0], right_pair[0])
    return (
        peak,
        left_pair[1] * jnp.exp(left_pair[0] - peak) + right_pair[1] * jnp.exp(right_pair[0] - peak),
    )


def local(points, potentials):
    link_index = lax.axis_index("link")
    link_count = lax.axis_size("link")
    tile_count = lax.axis_size("tile")
    per_link = (points.shape[0] - 1) // link_count
    cell_dev = points.shape[2]
    total_cells = tile_count * cell_dev
    offset_link = link_index * per_link
    local_pts = lax.dynamic_slice_in_dim(points, offset_link, per_link + 1, 0)
    local_pot = lax.dynamic_slice_in_dim(potentials, offset_link, per_link + 1, 0)
    every_pts = lax.all_gather(local_pts, "tile", axis=2, tiled=True)

    def message(source_idx, target_idx, source_msg):
        source_pts = local_pts[source_idx]
        target_pot = local_pot[target_idx]
        target_all = every_pts[target_idx]
        scores = pair_scores(source_pts, target_all, source_msg)
        peak = jnp.max(scores, axis=0)
        partial_lse = peak + jnp.log(jnp.sum(jnp.exp(scores - peak[None, :]), axis=0))
        lse_parts = lax.all_to_all(
            partial_lse.reshape(tile_count, cell_dev),
            "tile",
            split_axis=0,
            concat_axis=0,
            tiled=True,
        )
        peak = jnp.max(lse_parts, axis=0)
        summed = jnp.sum(jnp.exp(lse_parts - peak[None, :]), axis=0)
        return target_pot + peak + jnp.log(summed)

    def sweep(start_msg, forward):
        start_pos = jnp.where(forward, 0, per_link).astype(jnp.int32)
        stored = jnp.zeros((per_link + 1, cell_dev), jnp.float32)
        stored = lax.dynamic_update_slice_in_dim(stored, start_msg[None, :], start_pos, 0)
        current = start_msg
        for link_step in range(per_link):
            source_idx = jnp.where(forward, link_step, per_link - link_step).astype(jnp.int32)
            target_idx = jnp.where(forward, link_step + 1, per_link - 1 - link_step).astype(
                jnp.int32
            )
            current = message(source_idx, target_idx, current)
            stored = lax.dynamic_update_slice_in_dim(stored, current[None, :], target_idx, 0)
        return stored

    first_end = link_index == 0
    early_pass = sweep(local_pot[0], True)
    handed = passed_along(early_pass[per_link], "link", 1)
    forward_msgs = sweep(jnp.where(first_end, local_pot[0], handed), True)
    late_pass = sweep(local_pot[per_link], False)
    handed_back = passed_along(late_pass[0], "link", -1)
    backward_msgs = sweep(jnp.where(first_end, handed_back, local_pot[per_link]), False)
    combined = forward_msgs + backward_msgs - local_pot
    last_row = combined[per_link]
    peak = jnp.max(last_row)
    summed = jnp.sum(jnp.exp(last_row - peak))
    peak, summed = joined((peak, summed), "tile", combine_lse)
    log_total = peak + jnp.log(summed)
    return -math.log(total_cells) - (combined[1:] - log_total)


def fits(mesh, points):
    times, pcs, total = points.shape
    cell_dev = total // (mesh.shape["groups"] * mesh.shape["tile"])
    cells = cell_dev * mesh.shape["tile"]
    held = 2 * cells * cells * 4 + 2 * times * cells * 32 * 4
    return (
        cell_dev == 128
        and pcs < 32
        and times % 2 == 1
        and mesh.shape["tile"] % 2 == 0
        and cells % STRIP == 0
        and mesh.shape["link"] == 2
        and held < 32 * 1024 * 1024
    )


def solution(mesh):
    placed = (P(None, None, ("groups", "tile")), P(None, ("groups", "tile")))

    def whole(points, potentials):
        body = local_fast if fits(mesh, points) else local
        return jax.shard_map(
            body, mesh=mesh, in_specs=placed, out_specs=P("link", ("groups", "tile")), check_vma=False
        )(points, potentials)

    return whole
```

```python
import functools
import math

import jax
import jax.numpy as jnp
from jax import lax
from jax.experimental import pallas as pl
from jax.experimental.pallas import tpu as pltpu
from jax.sharding import PartitionSpec as P

EPSILON = 0.5
LOG2E = math.log2(math.e)
SCALE = 2.0 / EPSILON * LOG2E
STRIP = 1024
ROWS = 8
BLOCK = 64
WAYS = 2
DIRECT = 0


def pieces(value):
    high = value.astype(jnp.bfloat16)
    rest = value - high.astype(jnp.float32)
    middle = rest.astype(jnp.bfloat16)
    low = (rest - middle.astype(jnp.float32)).astype(jnp.bfloat16)
    return high, middle, low


def padded(points, extra):
    pad = 32 - points.shape[0]
    row = lax.broadcasted_iota(jnp.int32, (pad, points.shape[1]), 0)
    tail = jnp.where(row == 0, 0.0 if extra is None else extra, 0.0)
    return jnp.concatenate([points, tail], axis=0)


class Chain:
    def __init__(self, links, tiles, pts, pot, right, left, score, alpha, const, rest, col, own, tops, me, time):
        self.links, self.tiles = links, tiles
        self.pts, self.pot = pts, pot
        self.right, self.left, self.score = right, left, score
        self.alpha, self.const, self.rest = alpha, const, rest
        self.col, self.own, self.tops = col, own, tops
        self.me, self.time = me, time

    def constants(self, k, r):
        t = self.time(k)
        x = self.pts[t, r]
        lanes = pl.ds(pl.multiple_of(r * 128, 128), 128)
        square = jnp.sum(x * x, axis=0, keepdims=True)
        pot = self.pot[r, pl.ds(t, 1), :]
        self.const[t, :, lanes] = (pot - (2.0 / EPSILON) * square) * LOG2E
        if k == 0:
            self.alpha[t, :, lanes] = (pot - square / EPSILON) * LOG2E
        if k == self.links:
            self.rest[:, lanes] = square * (LOG2E / EPSILON)

    def prep_even(self, k, link, r):
        x = self.pts[self.time(k), r]
        one = jnp.full((1, 128), 1.0 if link % 2 == 0 else 0.0, jnp.float32)
        h, m, l = pieces(padded(x, one))
        zero = jnp.zeros_like(h)
        lanes = pl.ds(pl.multiple_of(r * 128, 128), 128)
        self.right[link % 2][:, lanes] = jnp.concatenate([h, h, h, m, l, m, zero, zero], axis=0)

    def prep_odd(self, k, r):
        t = self.time(k)
        lanes = pl.ds(pl.multiple_of(r * 128, 128), 128)
        x = padded(self.pts[t, r] * SCALE, self.const[t, :, lanes])
        h, m, l = pieces(x)
        block = jnp.concatenate([h, m, l, h], axis=0)
        block = block.T
        slot = (k // 2) % 2
        self.left[slot][lanes, 0:128] = block
        self.left[slot][lanes, 128:256] = block

    def prep(self, link, r):
        if link % 2 == 0:
            if link == 0:
                self.constants(0, r)
                self.prep_even(0, link, r)
            else:
                self.prep_even(link, link, r)
            self.constants(link + 1, r)
            self.prep_odd(link + 1, r)
        else:
            self.constants(link + 1, r)
            self.prep_even(link + 1, link, r)

    def product(self, link, i):
        lanes = pl.ds(pl.multiple_of(i * STRIP, STRIP), STRIP)
        slot = (link // 2) % 2
        self.score[link % 2][:, lanes] = jnp.dot(
            self.left[slot][...], self.right[link % 2][:, lanes], preferred_element_type=jnp.float32
        )

    def reduce_lanes(self, i):
        for j in range(STRIP // ROWS):
            rows = pl.ds(pl.multiple_of(i * STRIP + j * ROWS, ROWS), ROWS)
            top = self.tops[rows, :]
            peak = jnp.max(top, axis=1, keepdims=True)
            total = jnp.sum(self.col[rows, :] * jnp.exp2(top - peak), axis=1, keepdims=True)
            out = peak + jnp.log(total) * LOG2E
            self.col[rows, :] = jnp.broadcast_to(out, (ROWS, 128))

    def message(self, link, i):
        t = self.time(link)
        after = self.time(link + 1)
        if link % 2 == 0:
            source = self.alpha[t]
            rows = pl.ds(pl.multiple_of(i * STRIP, STRIP), STRIP)
            dots = jnp.dot(self.left[(link // 2) % 2][rows, :], self.right[0][...], preferred_element_type=jnp.float32)
            tiles = [slice(j * 128, (j + 1) * 128) for j in range(self.tiles)]
            for j in range(STRIP // ROWS):
                rows = pl.ds(pl.multiple_of(i * STRIP + j * ROWS, ROWS), ROWS)
                s = [dots[j * ROWS:(j + 1) * ROWS, c] + source[:, c] for c in tiles]
                top = functools.reduce(jnp.maximum, s)
                self.tops[rows, :] = top
                self.col[rows, :] = functools.reduce(jnp.add, [jnp.exp2(a - top) for a in s])
        else:
            lanes = pl.ds(pl.multiple_of(i * STRIP, STRIP), STRIP)
            cells = self.col.shape[0]
            step = BLOCK
            peak = total = None
            dots = jnp.dot(self.left[(link // 2) % 2][...], self.right[1][:, lanes], preferred_element_type=jnp.float32)
            for j in range(cells // step):
                rows = slice(j * step, (j + 1) * step)
                source = self.col[rows, :]
                s = dots[rows, :] + jnp.concatenate([source] * (STRIP // 128), axis=1)
                s = s.reshape(step // 8, 8, STRIP)
                top = jnp.max(s, axis=0)
                if peak is None:
                    peak = top
                    total = jnp.sum(jnp.exp2(s - peak[None]), axis=0)
                else:
                    new = jnp.maximum(peak, top)
                    total = total * jnp.exp2(peak - new) + jnp.sum(jnp.exp2(s - new[None]), axis=0)
                    peak = new
            top = jnp.max(peak, axis=0, keepdims=True)
            total = jnp.sum(total * jnp.exp2(peak - top), axis=0, keepdims=True)
            self.alpha[after, :, lanes] = self.const[after, :, lanes] + top + jnp.log(total) * LOG2E

    def keep(self, k):
        t = self.time(k)
        mine = pl.ds(pl.multiple_of(self.me * 128, 128), 128)
        if k % 2 == 0:
            self.own[t] = self.alpha[t, :, mine]
        else:
            block = self.col[mine, :]
            eye = lax.broadcasted_iota(jnp.int32, (128, 128), 0) == lax.broadcasted_iota(
                jnp.int32, (128, 128), 1
            )
            self.own[t] = jnp.sum(jnp.where(eye, block, 0.0), axis=0, keepdims=True)

    def log_total(self):
        phi = self.alpha[self.time(self.links)] + self.rest[...]
        peak = jnp.max(phi, axis=1, keepdims=True)
        return peak + jnp.log(jnp.sum(jnp.exp2(phi - peak), axis=1, keepdims=True)) * LOG2E

    def loop(self, count, body):
        def turn(i, carry):
            body(i)
            return carry

        lax.fori_loop(0, count, turn, 0)

    def whole(self, action):
        for r in range(self.tiles):
            action(r)

    def run(self, ready, done):
        half = self.links // 2
        ready(0)
        self.whole(lambda r: self.constants(0, r))
        self.whole(lambda r: self.prep_even(0, 0, r))
        ready(1)
        self.whole(lambda r: self.constants(1, r))
        self.whole(lambda r: self.prep_odd(1, r))
        for link in range(self.links):
            early = link + 1 < self.links and link >= half - 1
            if early:
                ready(link + 2)
            self.message(link, 0)
            if early:
                self.whole(lambda r: self.prep(link + 1, r))
            if link % 2 == 0:
                self.reduce_lanes(0)
            self.keep(link + 1)
            done(link + 1)
            if link + 1 < self.links and not early:
                ready(link + 2)
                self.whole(lambda r: self.prep(link + 1, r))


def chain_kernel(links, tiles, pts, pot, out, *scratch):
    held, pots, *pairs = scratch[:8]
    right, left, score = pairs[0:2], pairs[2:4], pairs[4:6]
    alpha, const, rest, col, own, other = scratch[8:14]
    line_send, line_recv, pair_send, pair_recv, core_send, core_recv, end_send, end_recv = scratch[14:22]
    fill, tops = scratch[22:]
    me = lax.axis_index("tile")
    way = lax.axis_index("link")
    line = tiles // 2
    at, side = me // 2, me % 2
    half = links // 2
    chunks = [(k, 1) for k in range(half + 1)]
    time = lambda k: k + way * (links - 2 * k)
    first = lambda k, count: k + way * (links - 2 * k - count + 1)
    slot = lambda z, y: 2 * z + y
    ahead = lambda d: slot(lax.rem(at + d, line), side)
    behind = lambda d: lax.rem(at + line - d, line)
    chain = Chain(
        links, tiles, held, pots, right, left, score, alpha, const, rest, col, own, tops, me, time
    )

    early = pl.ds(way * half, half + 1)
    mine = [
        pltpu.make_async_copy(pot, pots.at[me], fill.at[0]),
        pltpu.make_async_copy(pts.at[early], held.at[early, me], fill.at[1]),
    ]
    for copy in mine:
        copy.start()

    barrier = pltpu.get_barrier_semaphore()
    peers = [{"tile": ahead(d)} for d in range(1, line)]
    peers += [{"tile": slot(at, 1 - side)}, {"link": 1 - way}]
    for peer in peers:
        pl.semaphore_signal(barrier, inc=1, device_id=peer)
    pl.semaphore_wait(barrier, len(peers))

    def views(c, origin, source_own):
        if c == 0:
            return (pot if source_own else pots.at[origin]), pots.at[origin]
        k, count = chunks[c - 1]
        span = pl.ds(first(k, count), count)
        return (pts.at[span] if source_own else held.at[span, origin]), held.at[span, origin]

    def remote(c, origin, source_own, send, recv, d, device):
        src, dst = views(c, origin, source_own)
        return pltpu.make_async_remote_copy(
            src_ref=src,
            dst_ref=dst,
            send_sem=send.at[c, d],
            recv_sem=recv.at[c, d],
            device_id=device,
        )

    partner = {"tile": slot(at, 1 - side)}
    sent = []

    def to_line(c, d):
        copy = remote(c, me, True, line_send, line_recv, d, {"tile": ahead(d)})
        copy.start()
        sent.append(copy)

    def to_cross(c, d):
        device = {"tile": slot(lax.rem(at + d, line), 1 - side)}
        copy = remote(c, me, True, pair_send, pair_recv, d, device)
        copy.start()
        sent.append(copy)

    def to_pair(c, d):
        origin = slot(behind(d), side)
        copy = remote(c, origin, d == 0, pair_send, pair_recv, d, partner)
        copy.start()
        sent.append(copy)

    def forward(c):
        for d in range(1, line):
            origin = slot(behind(d), side)
            remote(c, origin, False, line_send, line_recv, d, partner).wait_recv()
            if c >= DIRECT:
                to_pair(c, d)

    def arrive(c):
        for d in range(line):
            origin = slot(behind(d), 1 - side)
            remote(c, origin, False, pair_send, pair_recv, d, partner).wait_recv()

    def across(k):
        t = time(k)
        copy = pltpu.make_async_remote_copy(
            src_ref=held.at[t],
            dst_ref=held.at[t],
            send_sem=core_send.at[k],
            recv_sem=core_recv.at[k],
            device_id={"link": 1 - way},
        )
        copy.start()
        sent.append(copy)

    def from_core(k):
        t = time(links - k)
        pltpu.make_async_remote_copy(
            src_ref=held.at[t],
            dst_ref=held.at[t],
            send_sem=core_send.at[k],
            recv_sem=core_recv.at[k],
            device_id={"link": 1 - way},
        ).wait_recv()

    def rows(which):
        return pl.ds(first(half, half), half) if which == 0 else pl.ds(time(links), 1)

    def ends(which, span):
        return pltpu.make_async_remote_copy(
            src_ref=own.at[span],
            dst_ref=other.at[span],
            send_sem=end_send.at[which],
            recv_sem=end_recv.at[which],
            device_id={"link": 1 - way},
        )

    for c in range(len(chunks) + 1):
        for d in range(line - 1, 0, -1):
            if c < DIRECT:
                to_cross(c, d)
            to_line(c, d)
        to_pair(c, 0)

    def ready(k):
        if k == 0:
            for copy in mine:
                copy.wait()
            for c in range(4):
                forward(c)
            for c in range(2):
                arrive(c)
            across(0)
        elif k <= half:
            if k + 3 <= half + 1:
                forward(k + 3)
            arrive(k + 1)
            if k < half:
                across(k)
        else:
            from_core(links - k)

    def done(k):
        if k == links - 1:
            copy = ends(0, rows(0))
            copy.start()
            sent.append(copy)
        if k == links:
            copy = ends(1, rows(1))
            copy.start()
            sent.append(copy)

    chain.run(ready, done)
    chain.keep(0)
    total = chain.log_total()
    last = sent.pop()
    for copy in sent:
        copy.wait_send()
    ends(0, rows_other(0, links, half, way)).wait_recv()
    ends(1, rows_other(1, links, half, way)).wait_recv()
    lanes = pl.ds(pl.multiple_of(me * 128, 128), 128)
    keep = -math.log(tiles * 128)
    for j in range(half):
        t = 1 + way * half + j
        combined = own[t] + other[t] - const[t, :, lanes]
        out[pl.ds(j, 1), :] = keep - (combined - total) / LOG2E
    last.wait_send()


def rows_other(which, links, half, way):
    back = 1 - way
    if which == 0:
        return pl.ds(half + back * (1 - half), half)
    return pl.ds(links - back * links, 1)


def local_fast(points, potentials):
    times, pcs, cell_dev = points.shape
    links = times - 1
    tiles = lax.axis_size("tile")
    cells = tiles * cell_dev
    vmem = pl.BlockSpec(memory_space=pltpu.VMEM)
    hbm = pl.BlockSpec(memory_space=pltpu.HBM)
    dma = pltpu.SemaphoreType.DMA
    phases = links // 2 + 2
    line = tiles // 2
    return pl.pallas_call(
        functools.partial(chain_kernel, links, tiles),
        out_shape=jax.ShapeDtypeStruct((links // 2, 128), jnp.float32),
        in_specs=[hbm] * 2,
        out_specs=vmem,
        scratch_shapes=[
            pltpu.VMEM((times, tiles, pcs, 128), jnp.float32),
            pltpu.VMEM((tiles, times, 128), jnp.float32),
            pltpu.VMEM((256, cells), jnp.bfloat16),
            pltpu.VMEM((256, cells), jnp.bfloat16),
            pltpu.VMEM((cells, 256), jnp.bfloat16),
            pltpu.VMEM((cells, 256), jnp.bfloat16),
            pltpu.VMEM((cells, cells), jnp.float32),
            pltpu.VMEM((cells, cells), jnp.float32),
            pltpu.VMEM((times, 1, cells), jnp.float32),
            pltpu.VMEM((times, 1, cells), jnp.float32),
            pltpu.VMEM((1, cells), jnp.float32),
            pltpu.VMEM((cells, 128), jnp.float32),
            pltpu.VMEM((times, 1, 128), jnp.float32),
            pltpu.VMEM((times, 1, 128), jnp.float32),
            dma((phases, line)),
            dma((phases, line)),
            dma((phases, line)),
            dma((phases, line)),
            dma((links // 2,)),
            dma((links // 2,)),
            dma((2,)),
            dma((2,)),
            dma((2,)),
            pltpu.VMEM((cells, 128), jnp.float32),
        ],
        compiler_params=pltpu.CompilerParams(
            vmem_limit_bytes=66900000, collective_id=0, has_side_effects=True
        ),
    )(points, potentials)


def passed_along(block, axis, distance):
    devices = range(lax.axis_size(axis))
    route = [(i - distance, i) for i in devices if i - distance in devices]
    return lax.ppermute(block, axis, route)


def joined(part, axis, combine):
    gathered = jax.tree.map(lambda a: lax.all_gather(a, axis), part)

    def take(source):
        return jax.tree.map(lambda a: lax.dynamic_index_in_dim(a, source, 0, False), gathered)

    return lax.fori_loop(
        1, lax.axis_size(axis), lambda source, state: combine(state, take(source)), take(0)
    )


def pair_scores(source_pts, target_pts, source_msg):
    source_sq = jnp.sum(source_pts * source_pts, axis=0)
    target_sq = jnp.sum(target_pts * target_pts, axis=0)
    inner_prod = lax.dot_general(
        source_pts,
        target_pts,
        (((0,), (0,)), ((), ())),
        precision=lax.Precision.HIGHEST,
        preferred_element_type=jnp.float32,
    )
    pair_cost = source_sq[:, None] + target_sq[None, :] - 2.0 * inner_prod
    return source_msg[:, None] - pair_cost / EPSILON


def combine_lse(left_pair, right_pair):
    peak = jnp.maximum(left_pair[0], right_pair[0])
    return (
        peak,
        left_pair[1] * jnp.exp(left_pair[0] - peak) + right_pair[1] * jnp.exp(right_pair[0] - peak),
    )


def local(points, potentials):
    link_index = lax.axis_index("link")
    link_count = lax.axis_size("link")
    tile_count = lax.axis_size("tile")
    per_link = (points.shape[0] - 1) // link_count
    cell_dev = points.shape[2]
    total_cells = tile_count * cell_dev
    offset_link = link_index * per_link
    local_pts = lax.dynamic_slice_in_dim(points, offset_link, per_link + 1, 0)
    local_pot = lax.dynamic_slice_in_dim(potentials, offset_link, per_link + 1, 0)
    every_pts = lax.all_gather(local_pts, "tile", axis=2, tiled=True)

    def message(source_idx, target_idx, source_msg):
        source_pts = local_pts[source_idx]
        target_pot = local_pot[target_idx]
        target_all = every_pts[target_idx]
        scores = pair_scores(source_pts, target_all, source_msg)
        peak = jnp.max(scores, axis=0)
        partial_lse = peak + jnp.log(jnp.sum(jnp.exp(scores - peak[None, :]), axis=0))
        lse_parts = lax.all_to_all(
            partial_lse.reshape(tile_count, cell_dev),
            "tile",
            split_axis=0,
            concat_axis=0,
            tiled=True,
        )
        peak = jnp.max(lse_parts, axis=0)
        summed = jnp.sum(jnp.exp(lse_parts - peak[None, :]), axis=0)
        return target_pot + peak + jnp.log(summed)

    def sweep(start_msg, forward):
        start_pos = jnp.where(forward, 0, per_link).astype(jnp.int32)
        stored = jnp.zeros((per_link + 1, cell_dev), jnp.float32)
        stored = lax.dynamic_update_slice_in_dim(stored, start_msg[None, :], start_pos, 0)
        current = start_msg
        for link_step in range(per_link):
            source_idx = jnp.where(forward, link_step, per_link - link_step).astype(jnp.int32)
            target_idx = jnp.where(forward, link_step + 1, per_link - 1 - link_step).astype(
                jnp.int32
            )
            current = message(source_idx, target_idx, current)
            stored = lax.dynamic_update_slice_in_dim(stored, current[None, :], target_idx, 0)
        return stored

    first_end = link_index == 0
    early_pass = sweep(local_pot[0], True)
    handed = passed_along(early_pass[per_link], "link", 1)
    forward_msgs = sweep(jnp.where(first_end, local_pot[0], handed), True)
    late_pass = sweep(local_pot[per_link], False)
    handed_back = passed_along(late_pass[0], "link", -1)
    backward_msgs = sweep(jnp.where(first_end, handed_back, local_pot[per_link]), False)
    combined = forward_msgs + backward_msgs - local_pot
    last_row = combined[per_link]
    peak = jnp.max(last_row)
    summed = jnp.sum(jnp.exp(last_row - peak))
    peak, summed = joined((peak, summed), "tile", combine_lse)
    log_total = peak + jnp.log(summed)
    return -math.log(total_cells) - (combined[1:] - log_total)


def fits(mesh, points):
    times, pcs, total = points.shape
    cell_dev = total // (mesh.shape["groups"] * mesh.shape["tile"])
    cells = cell_dev * mesh.shape["tile"]
    held = 2 * cells * cells * 4 + 2 * times * cells * 32 * 4
    return (
        cell_dev == 128
        and pcs < 32
        and times % 2 == 1
        and mesh.shape["tile"] % 2 == 0
        and cells % STRIP == 0
        and mesh.shape["link"] == 2
        and held < 32 * 1024 * 1024
    )


def solution(mesh):
    placed = (P(None, None, ("groups", "tile")), P(None, ("groups", "tile")))

    def whole(points, potentials):
        body = local_fast if fits(mesh, points) else local
        return jax.shard_map(
            body, mesh=mesh, in_specs=placed, out_specs=P("link", ("groups", "tile")), check_vma=False
        )(points, potentials)

    return whole
```

```python
import functools
import math

import jax
import jax.numpy as jnp
from jax import lax
from jax.experimental import pallas as pl
from jax.experimental.pallas import tpu as pltpu
from jax.sharding import PartitionSpec as P

EPSILON = 0.5
LOG2E = math.log2(math.e)
SCALE = 2.0 / EPSILON * LOG2E
STRIP = 1024
ROWS = 8
BLOCK = 64
BAND = 256


def pieces(value):
    high = value.astype(jnp.bfloat16)
    rest = value - high.astype(jnp.float32)
    middle = rest.astype(jnp.bfloat16)
    low = (rest - middle.astype(jnp.float32)).astype(jnp.bfloat16)
    return high, middle, low


def padded(points, extra):
    pad = 32 - points.shape[0]
    row = lax.broadcasted_iota(jnp.int32, (pad, points.shape[1]), 0)
    tail = jnp.where(row == 0, 0.0 if extra is None else extra, 0.0)
    return jnp.concatenate([points, tail], axis=0)


class Chain:
    def __init__(self, links, tiles, pcs, pts, right, left, score, alpha, const, rest, col, own, tops, at, place, time):
        self.links, self.tiles = links, tiles
        self.pts, self.pcs = pts, pcs
        self.right, self.left, self.score = right, left, score
        self.alpha, self.const, self.rest = alpha, const, rest
        self.col, self.own, self.tops = col, own, tops
        self.at, self.place, self.time = at, place, time

    def constants(self, k, r):
        t = self.time(k)
        x = self.pts[t, self.place(r), : self.pcs]
        lanes = pl.ds(pl.multiple_of(r * 128, 128), 128)
        square = jnp.sum(x * x, axis=0, keepdims=True)
        pot = self.pts[t, self.place(r), self.pcs :]
        self.const[t, :, lanes] = (pot - (2.0 / EPSILON) * square) * LOG2E
        if k == 0:
            self.alpha[t, :, lanes] = (pot - square / EPSILON) * LOG2E
        if k == self.links:
            self.rest[:, lanes] = square * (LOG2E / EPSILON)

    def prep_even(self, k, link, r):
        x = self.pts[self.time(k), self.place(r), : self.pcs]
        one = jnp.full((1, 128), 1.0 if link % 2 == 0 else 0.0, jnp.float32)
        h, m, l = pieces(padded(x, one))
        zero = jnp.zeros_like(h)
        lanes = pl.ds(pl.multiple_of(r * 128, 128), 128)
        self.right[link % 2][:, lanes] = jnp.concatenate([h, h, h, m, l, m, zero, zero], axis=0)

    def prep_odd(self, k, r):
        t = self.time(k)
        lanes = pl.ds(pl.multiple_of(r * 128, 128), 128)
        x = padded(self.pts[t, self.place(r), : self.pcs] * SCALE, self.const[t, :, lanes])
        h, m, l = pieces(x)
        block = jnp.concatenate([h, m, l, h], axis=0)
        block = block.T
        slot = (k // 2) % 2
        self.left[slot][lanes, 0:128] = block
        self.left[slot][lanes, 128:256] = block

    def prep(self, link, r):
        if link % 2 == 0:
            if link == 0:
                self.constants(0, r)
                self.prep_even(0, link, r)
            else:
                self.prep_even(link, link, r)
            self.constants(link + 1, r)
            self.prep_odd(link + 1, r)
        else:
            self.constants(link + 1, r)
            self.prep_even(link + 1, link, r)

    def product(self, link, i):
        lanes = pl.ds(pl.multiple_of(i * STRIP, STRIP), STRIP)
        slot = (link // 2) % 2
        self.score[link % 2][:, lanes] = jnp.dot(
            self.left[slot][...], self.right[link % 2][:, lanes], preferred_element_type=jnp.float32
        )

    def reduce_lanes(self, i):
        for j in range(STRIP // ROWS):
            rows = pl.ds(pl.multiple_of(i * STRIP + j * ROWS, ROWS), ROWS)
            top = self.tops[rows, :]
            peak = jnp.max(top, axis=1, keepdims=True)
            total = jnp.sum(self.col[rows, :] * jnp.exp2(top - peak), axis=1, keepdims=True)
            out = peak + jnp.log(total) * LOG2E
            self.col[rows, :] = jnp.broadcast_to(out, (ROWS, 128))

    def partial(self, link, rows, tiles, first):
        source = self.alpha[self.time(link)]
        lanes = slice(tiles[0] * 128, tiles[-1] * 128 + 128)
        for low in range(rows.start, rows.stop, BAND):
            dots = jnp.dot(
                self.left[(link // 2) % 2][low:low + BAND, :],
                self.right[0][:, lanes],
                preferred_element_type=jnp.float32,
            )
            for j in range(0, BAND, ROWS):
                here = slice(low + j, low + j + ROWS)
                s = [
                    dots[j:j + ROWS, n * 128:n * 128 + 128] + source[:, c * 128:c * 128 + 128]
                    for n, c in enumerate(tiles)
                ]
                top = functools.reduce(jnp.maximum, s)
                if not first:
                    old = self.tops[here, :]
                    top = jnp.maximum(top, old)
                total = functools.reduce(jnp.add, [jnp.exp2(a - top) for a in s])
                if not first:
                    total = total + self.col[here, :] * jnp.exp2(old - top)
                self.tops[here, :] = top
                self.col[here, :] = total

    def message(self, link, i):
        after = self.time(link + 1)
        if link % 2 == 0:
            self.partial(link, slice(0, self.tiles * 128), range(self.tiles), True)
        else:
            lanes = pl.ds(pl.multiple_of(i * STRIP, STRIP), STRIP)
            cells = self.col.shape[0]
            step = BLOCK
            peak = total = None
            dots = jnp.dot(self.left[(link // 2) % 2][...], self.right[1][:, lanes], preferred_element_type=jnp.float32)
            for j in range(cells // step):
                rows = slice(j * step, (j + 1) * step)
                source = self.col[rows, :]
                s = dots[rows, :] + jnp.concatenate([source] * (STRIP // 128), axis=1)
                s = s.reshape(step // 8, 8, STRIP)
                top = jnp.max(s, axis=0)
                if peak is None:
                    peak = top
                    total = jnp.sum(jnp.exp2(s - peak[None]), axis=0)
                else:
                    new = jnp.maximum(peak, top)
                    total = total * jnp.exp2(peak - new) + jnp.sum(jnp.exp2(s - new[None]), axis=0)
                    peak = new
            top = jnp.max(peak, axis=0, keepdims=True)
            total = jnp.sum(total * jnp.exp2(peak - top), axis=0, keepdims=True)
            self.alpha[after, :, lanes] = self.const[after, :, lanes] + top + jnp.log(total) * LOG2E

    def keep(self, k):
        t = self.time(k)
        mine = pl.ds(pl.multiple_of(self.at * 128, 128), 128)
        if k % 2 == 0:
            self.own[t] = self.alpha[t, :, mine]
        else:
            block = self.col[mine, :]
            eye = lax.broadcasted_iota(jnp.int32, (128, 128), 0) == lax.broadcasted_iota(
                jnp.int32, (128, 128), 1
            )
            self.own[t] = jnp.sum(jnp.where(eye, block, 0.0), axis=0, keepdims=True)

    def log_total(self):
        phi = self.alpha[self.time(self.links)] + self.rest[...]
        peak = jnp.max(phi, axis=1, keepdims=True)
        return peak + jnp.log(jnp.sum(jnp.exp2(phi - peak), axis=1, keepdims=True)) * LOG2E

    def loop(self, count, body):
        def turn(i, carry):
            body(i)
            return carry

        lax.fori_loop(0, count, turn, 0)

    def whole(self, action, low=0, high=None):
        for r in range(low, self.tiles if high is None else high):
            action(r)

    def run(self, ready, done):
        half = self.links // 2
        line = self.tiles // 2
        near, far = slice(0, line * 128), slice(line * 128, self.tiles * 128)
        ready(0)
        self.whole(lambda r: self.constants(0, r), high=line)
        self.whole(lambda r: self.prep_even(0, 0, r), high=line)
        self.whole(lambda r: self.constants(1, r), high=line)
        self.whole(lambda r: self.prep_odd(1, r), high=line)
        self.partial(0, near, range(line), True)
        ready("sources")
        self.whole(lambda r: self.constants(0, r), low=line)
        self.whole(lambda r: self.prep_even(0, 0, r), low=line)
        self.partial(0, near, range(line, self.tiles), False)
        ready(1)
        self.whole(lambda r: self.constants(1, r), low=line)
        self.whole(lambda r: self.prep_odd(1, r), low=line)
        self.partial(0, far, range(self.tiles), True)
        for link in range(self.links):
            early = link + 1 < self.links and link >= half - 1
            if early:
                ready(link + 2)
            if link:
                self.message(link, 0)
            if early:
                self.whole(lambda r: self.prep(link + 1, r))
            if link % 2 == 0:
                self.reduce_lanes(0)
            self.keep(link + 1)
            done(link + 1)
            if link + 1 < self.links and not early:
                ready(link + 2)
                self.whole(lambda r: self.prep(link + 1, r))


def chain_kernel(links, tiles, pts, pot, out, *scratch):
    held, *pairs = scratch[:7]
    right, left, score = pairs[0:2], pairs[2:4], pairs[4:6]
    alpha, const, rest, col, own, other = scratch[7:13]
    line_send, line_recv, pair_send, pair_recv, core_send, core_recv, end_send, end_recv = scratch[13:21]
    fill, tops, own_pts, own_pot, stage = scratch[21:]
    me = lax.axis_index("tile")
    way = lax.axis_index("link")
    line = tiles // 2
    at, side = me // 2, me % 2
    half = links // 2
    chunks = [(k, 1) for k in range(half + 1)]
    time = lambda k: k + way * (links - 2 * k)
    first = lambda k, count: k + way * (links - 2 * k - count + 1)
    slot = lambda z, y: 2 * z + y
    place = lambda r: slot(r % line, side if r < line else 1 - side)
    ahead = lambda d: slot(lax.rem(at + d, line), side)
    behind = lambda d: lax.rem(at + line - d, line)
    chain = Chain(
        links, tiles, pts.shape[1], held, right, left, score, alpha, const, rest, col, own, tops, at, place, time
    )

    early = pl.ds(way * half, half + 1)
    mine = [
        pltpu.make_async_copy(pot, own_pot, fill.at[0]),
        pltpu.make_async_copy(pts.at[early], own_pts, fill.at[1]),
    ]
    for copy in mine:
        copy.start()

    barrier = pltpu.get_barrier_semaphore()
    peers = [{"tile": ahead(d)} for d in range(1, line)]
    peers += [{"tile": slot(at, 1 - side)}, {"link": 1 - way}]
    for peer in peers:
        pl.semaphore_signal(barrier, inc=1, device_id=peer)
    for copy in mine:
        copy.wait()
    for j in range(half + 1):
        t = way * half + j
        block = jnp.concatenate([own_pts[j], own_pot[pl.ds(t, 1), :]], axis=0)
        stage[j] = block
        held[t, me] = block
    pl.semaphore_wait(barrier, len(peers))

    def views(c, origin, source_own):
        k, count = chunks[c]
        span = pl.ds(first(k, count), count)
        part = pl.ds(first(k, count) - way * half, count)
        return (stage.at[part] if source_own else held.at[span, origin]), held.at[span, origin]

    def remote(c, origin, source_own, send, recv, d, device):
        src, dst = views(c, origin, source_own)
        return pltpu.make_async_remote_copy(
            src_ref=src,
            dst_ref=dst,
            send_sem=send.at[c, d],
            recv_sem=recv.at[c, d],
            device_id=device,
        )

    partner = {"tile": slot(at, 1 - side)}
    sent = []

    def to_line(c, d):
        copy = remote(c, me, True, line_send, line_recv, d, {"tile": ahead(d)})
        copy.start()
        sent.append(copy)

    def to_pair(c, d):
        origin = slot(behind(d), side)
        copy = remote(c, origin, d == 0, pair_send, pair_recv, d, partner)
        copy.start()
        sent.append(copy)

    def forward(c):
        for d in range(1, line):
            origin = slot(behind(d), side)
            remote(c, origin, False, line_send, line_recv, d, partner).wait_recv()
            to_pair(c, d)

    def arrive(c):
        for d in range(line):
            origin = slot(behind(d), 1 - side)
            remote(c, origin, False, pair_send, pair_recv, d, partner).wait_recv()

    def across(k):
        t = time(k)
        copy = pltpu.make_async_remote_copy(
            src_ref=held.at[t],
            dst_ref=held.at[t],
            send_sem=core_send.at[k],
            recv_sem=core_recv.at[k],
            device_id={"link": 1 - way},
        )
        copy.start()
        sent.append(copy)

    def from_core(k):
        t = time(links - k)
        pltpu.make_async_remote_copy(
            src_ref=held.at[t],
            dst_ref=held.at[t],
            send_sem=core_send.at[k],
            recv_sem=core_recv.at[k],
            device_id={"link": 1 - way},
        ).wait_recv()

    def rows(which):
        return pl.ds(first(half, half), half) if which == 0 else pl.ds(time(links), 1)

    def ends(which, span):
        return pltpu.make_async_remote_copy(
            src_ref=own.at[span],
            dst_ref=other.at[span],
            send_sem=end_send.at[which],
            recv_sem=end_recv.at[which],
            device_id={"link": 1 - way},
        )

    for c in range(len(chunks)):
        for d in range(line - 1, 0, -1):
            to_line(c, d)
        to_pair(c, 0)

    def ready(k):
        if k == 0:
            for c in range(3):
                forward(c)
        elif k == "sources":
            arrive(0)
            across(0)
        elif k <= half:
            if k + 2 <= half:
                forward(k + 2)
            arrive(k)
            if k < half:
                across(k)
        elif k == half + 1:
            for c in range(half - 1, -1, -1):
                from_core(c)

    def done(k):
        if k == links:
            for which in range(2):
                copy = ends(which, rows(which))
                copy.start()
                sent.append(copy)

    chain.run(ready, done)
    chain.keep(0)
    total = chain.log_total()
    last = [sent.pop(), sent.pop()]
    for copy in sent:
        copy.wait_send()
    ends(0, rows_other(0, links, half, way)).wait_recv()
    ends(1, rows_other(1, links, half, way)).wait_recv()
    lanes = pl.ds(pl.multiple_of(at * 128, 128), 128)
    keep = -math.log(tiles * 128)
    for j in range(half):
        t = 1 + way * half + j
        combined = own[t] + other[t] - const[t, :, lanes]
        out[pl.ds(j, 1), :] = keep - (combined - total) / LOG2E
    for copy in last:
        copy.wait_send()


def rows_other(which, links, half, way):
    back = 1 - way
    if which == 0:
        return pl.ds(half + back * (1 - half), half)
    return pl.ds(links - back * links, 1)


def local_fast(points, potentials):
    times, pcs, cell_dev = points.shape
    links = times - 1
    tiles = lax.axis_size("tile")
    cells = tiles * cell_dev
    vmem = pl.BlockSpec(memory_space=pltpu.VMEM)
    hbm = pl.BlockSpec(memory_space=pltpu.HBM)
    dma = pltpu.SemaphoreType.DMA
    phases = links // 2 + 1
    line = tiles // 2
    return pl.pallas_call(
        functools.partial(chain_kernel, links, tiles),
        out_shape=jax.ShapeDtypeStruct((links // 2, 128), jnp.float32),
        in_specs=[hbm] * 2,
        out_specs=vmem,
        scratch_shapes=[
            pltpu.VMEM((times, tiles, pcs + 1, 128), jnp.float32),
            pltpu.VMEM((256, cells), jnp.bfloat16),
            pltpu.VMEM((256, cells), jnp.bfloat16),
            pltpu.VMEM((cells, 256), jnp.bfloat16),
            pltpu.VMEM((cells, 256), jnp.bfloat16),
            pltpu.VMEM((cells, cells), jnp.float32),
            pltpu.VMEM((cells, cells), jnp.float32),
            pltpu.VMEM((times, 1, cells), jnp.float32),
            pltpu.VMEM((times, 1, cells), jnp.float32),
            pltpu.VMEM((1, cells), jnp.float32),
            pltpu.VMEM((cells, 128), jnp.float32),
            pltpu.VMEM((times, 1, 128), jnp.float32),
            pltpu.VMEM((times, 1, 128), jnp.float32),
            dma((phases, line)),
            dma((phases, line)),
            dma((phases, line)),
            dma((phases, line)),
            dma((links // 2,)),
            dma((links // 2,)),
            dma((2,)),
            dma((2,)),
            dma((2,)),
            pltpu.VMEM((cells, 128), jnp.float32),
            pltpu.VMEM((links // 2 + 1, pcs, 128), jnp.float32),
            pltpu.VMEM((times, 128), jnp.float32),
            pltpu.VMEM((links // 2 + 1, pcs + 1, 128), jnp.float32),
        ],
        compiler_params=pltpu.CompilerParams(
            vmem_limit_bytes=66900000, collective_id=0, has_side_effects=True
        ),
    )(points, potentials)


def passed_along(block, axis, distance):
    devices = range(lax.axis_size(axis))
    route = [(i - distance, i) for i in devices if i - distance in devices]
    return lax.ppermute(block, axis, route)


def joined(part, axis, combine):
    gathered = jax.tree.map(lambda a: lax.all_gather(a, axis), part)

    def take(source):
        return jax.tree.map(lambda a: lax.dynamic_index_in_dim(a, source, 0, False), gathered)

    return lax.fori_loop(
        1, lax.axis_size(axis), lambda source, state: combine(state, take(source)), take(0)
    )


def pair_scores(source_pts, target_pts, source_msg):
    source_sq = jnp.sum(source_pts * source_pts, axis=0)
    target_sq = jnp.sum(target_pts * target_pts, axis=0)
    inner_prod = lax.dot_general(
        source_pts,
        target_pts,
        (((0,), (0,)), ((), ())),
        precision=lax.Precision.HIGHEST,
        preferred_element_type=jnp.float32,
    )
    pair_cost = source_sq[:, None] + target_sq[None, :] - 2.0 * inner_prod
    return source_msg[:, None] - pair_cost / EPSILON


def combine_lse(left_pair, right_pair):
    peak = jnp.maximum(left_pair[0], right_pair[0])
    return (
        peak,
        left_pair[1] * jnp.exp(left_pair[0] - peak) + right_pair[1] * jnp.exp(right_pair[0] - peak),
    )


def local(points, potentials):
    link_index = lax.axis_index("link")
    link_count = lax.axis_size("link")
    tile_count = lax.axis_size("tile")
    per_link = (points.shape[0] - 1) // link_count
    cell_dev = points.shape[2]
    total_cells = tile_count * cell_dev
    offset_link = link_index * per_link
    local_pts = lax.dynamic_slice_in_dim(points, offset_link, per_link + 1, 0)
    local_pot = lax.dynamic_slice_in_dim(potentials, offset_link, per_link + 1, 0)
    every_pts = lax.all_gather(local_pts, "tile", axis=2, tiled=True)

    def message(source_idx, target_idx, source_msg):
        source_pts = local_pts[source_idx]
        target_pot = local_pot[target_idx]
        target_all = every_pts[target_idx]
        scores = pair_scores(source_pts, target_all, source_msg)
        peak = jnp.max(scores, axis=0)
        partial_lse = peak + jnp.log(jnp.sum(jnp.exp(scores - peak[None, :]), axis=0))
        lse_parts = lax.all_to_all(
            partial_lse.reshape(tile_count, cell_dev),
            "tile",
            split_axis=0,
            concat_axis=0,
            tiled=True,
        )
        peak = jnp.max(lse_parts, axis=0)
        summed = jnp.sum(jnp.exp(lse_parts - peak[None, :]), axis=0)
        return target_pot + peak + jnp.log(summed)

    def sweep(start_msg, forward):
        start_pos = jnp.where(forward, 0, per_link).astype(jnp.int32)
        stored = jnp.zeros((per_link + 1, cell_dev), jnp.float32)
        stored = lax.dynamic_update_slice_in_dim(stored, start_msg[None, :], start_pos, 0)
        current = start_msg
        for link_step in range(per_link):
            source_idx = jnp.where(forward, link_step, per_link - link_step).astype(jnp.int32)
            target_idx = jnp.where(forward, link_step + 1, per_link - 1 - link_step).astype(
                jnp.int32
            )
            current = message(source_idx, target_idx, current)
            stored = lax.dynamic_update_slice_in_dim(stored, current[None, :], target_idx, 0)
        return stored

    first_end = link_index == 0
    early_pass = sweep(local_pot[0], True)
    handed = passed_along(early_pass[per_link], "link", 1)
    forward_msgs = sweep(jnp.where(first_end, local_pot[0], handed), True)
    late_pass = sweep(local_pot[per_link], False)
    handed_back = passed_along(late_pass[0], "link", -1)
    backward_msgs = sweep(jnp.where(first_end, handed_back, local_pot[per_link]), False)
    combined = forward_msgs + backward_msgs - local_pot
    last_row = combined[per_link]
    peak = jnp.max(last_row)
    summed = jnp.sum(jnp.exp(last_row - peak))
    peak, summed = joined((peak, summed), "tile", combine_lse)
    log_total = peak + jnp.log(summed)
    return -math.log(total_cells) - (combined[1:] - log_total)


def fits(mesh, points):
    times, pcs, total = points.shape
    cell_dev = total // (mesh.shape["groups"] * mesh.shape["tile"])
    cells = cell_dev * mesh.shape["tile"]
    held = 2 * cells * cells * 4 + 2 * times * cells * 32 * 4
    return (
        cell_dev == 128
        and pcs < 32
        and times % 2 == 1
        and mesh.shape["tile"] % 2 == 0
        and cells % STRIP == 0
        and mesh.shape["link"] == 2
        and held < 32 * 1024 * 1024
    )


def solution(mesh):
    placed = (P(None, None, ("groups", "tile")), P(None, ("groups", "tile")))

    def whole(points, potentials):
        body = local_fast if fits(mesh, points) else local
        return jax.shard_map(
            body, mesh=mesh, in_specs=placed, out_specs=P("link", ("groups", "tile")), check_vma=False
        )(points, potentials)

    return whole
```

```python
import functools
import math

import jax
import jax.numpy as jnp
from jax import lax
from jax.experimental import pallas as pl
from jax.experimental.pallas import tpu as pltpu
from jax.sharding import PartitionSpec as P

EPSILON = 0.5
LOG2E = math.log2(math.e)
SCALE = 2.0 / EPSILON * LOG2E
STRIP = 1024
ROWS = 8
BLOCK = 64
BAND = 256


def pieces(value):
    high = value.astype(jnp.bfloat16)
    rest = value - high.astype(jnp.float32)
    middle = rest.astype(jnp.bfloat16)
    low = (rest - middle.astype(jnp.float32)).astype(jnp.bfloat16)
    return high, middle, low


def padded(points, extra, slot):
    pad = 32 - points.shape[0]
    row = lax.broadcasted_iota(jnp.int32, (pad, points.shape[1]), 0)
    tail = jnp.where(row == slot, extra, 0.0)
    return jnp.concatenate([points, tail], axis=0)


class Chain:
    def __init__(self, links, tiles, pcs, pts, right, left, alpha, const, rest, col, own, tops, at, place, time):
        self.links, self.tiles = links, tiles
        self.pts, self.pcs = pts, pcs
        self.right, self.left = right, left
        self.alpha, self.const, self.rest = alpha, const, rest
        self.col, self.own, self.tops = col, own, tops
        self.at, self.place, self.time = at, place, time

    def constants(self, k, r):
        t = self.time(k)
        x = self.pts[t, self.place(r), : self.pcs]
        lanes = pl.ds(pl.multiple_of(r * 128, 128), 128)
        square = jnp.sum(x * x, axis=0, keepdims=True)
        pot = self.pts[t, self.place(r), self.pcs :]
        self.const[t, :, lanes] = (pot - (2.0 / EPSILON) * square) * LOG2E
        if k == 0:
            self.alpha[t, :, lanes] = (pot - square / EPSILON) * LOG2E
        if k == self.links:
            self.rest[:, lanes] = square * (LOG2E / EPSILON)

    def prep_even(self, k, r):
        slot = (k // 2) % 2
        x = self.pts[self.time(k), self.place(r), : self.pcs]
        h, m, l = pieces(padded(x, jnp.ones((1, 128), jnp.float32), slot))
        lanes = pl.ds(pl.multiple_of(r * 128, 128), 128)
        self.right[slot][0:192, lanes] = jnp.concatenate([h, h, h, m, l, m], axis=0)

    def prep_odd(self, k, r):
        slot = (k // 2) % 2
        t = self.time(k)
        lanes = pl.ds(pl.multiple_of(r * 128, 128), 128)
        x = self.pts[t, self.place(r), : self.pcs] * SCALE
        h, m, l = pieces(padded(x, self.const[t, :, lanes], slot))
        block = jnp.concatenate([h, m, l, h], axis=0)
        block = block.T
        self.left[slot][lanes, 0:128] = block
        self.left[slot][lanes, 128:256] = block

    def prep(self, link, r):
        self.constants(link + 1, r)
        if link % 2 == 0:
            self.prep_odd(link + 1, r)
        else:
            self.prep_even(link + 1, r)

    def reduce_lanes(self, i):
        for j in range(STRIP // ROWS):
            rows = pl.ds(pl.multiple_of(i * STRIP + j * ROWS, ROWS), ROWS)
            top = self.tops[rows, :]
            peak = jnp.max(top, axis=1, keepdims=True)
            total = jnp.sum(self.col[rows, :] * jnp.exp2(top - peak), axis=1, keepdims=True)
            out = peak + jnp.log(total) * LOG2E
            self.col[rows, :] = jnp.broadcast_to(out, (ROWS, 128))

    def partial(self, link, rows, tiles, first):
        source = self.alpha[self.time(link)]
        lanes = slice(tiles[0] * 128, tiles[-1] * 128 + 128)
        for low in range(rows.start, rows.stop, BAND):
            dots = jnp.dot(
                self.left[(link // 2) % 2][low:low + BAND, :],
                self.right[(link // 2) % 2][:, lanes],
                preferred_element_type=jnp.float32,
            )
            for j in range(0, BAND, ROWS):
                here = slice(low + j, low + j + ROWS)
                s = [
                    dots[j:j + ROWS, n * 128:n * 128 + 128] + source[:, c * 128:c * 128 + 128]
                    for n, c in enumerate(tiles)
                ]
                top = functools.reduce(jnp.maximum, s)
                if not first:
                    old = self.tops[here, :]
                    top = jnp.maximum(top, old)
                total = functools.reduce(jnp.add, [jnp.exp2(a - top) for a in s])
                if not first:
                    total = total + self.col[here, :] * jnp.exp2(old - top)
                self.tops[here, :] = top
                self.col[here, :] = total

    def message(self, link, i):
        after = self.time(link + 1)
        if link % 2 == 0:
            self.partial(link, slice(0, self.tiles * 128), range(self.tiles), True)
        else:
            lanes = pl.ds(pl.multiple_of(i * STRIP, STRIP), STRIP)
            cells = self.col.shape[0]
            step = BLOCK
            peak = total = None
            dots = jnp.dot(self.left[(link // 2) % 2][...], self.right[((link + 1) // 2) % 2][:, lanes], preferred_element_type=jnp.float32)
            for j in range(cells // step):
                rows = slice(j * step, (j + 1) * step)
                source = self.col[rows, :]
                s = dots[rows, :] + jnp.concatenate([source] * (STRIP // 128), axis=1)
                s = s.reshape(step // 8, 8, STRIP)
                top = jnp.max(s, axis=0)
                if peak is None:
                    peak = top
                    total = jnp.sum(jnp.exp2(s - peak[None]), axis=0)
                else:
                    new = jnp.maximum(peak, top)
                    total = total * jnp.exp2(peak - new) + jnp.sum(jnp.exp2(s - new[None]), axis=0)
                    peak = new
            top = jnp.max(peak, axis=0, keepdims=True)
            total = jnp.sum(total * jnp.exp2(peak - top), axis=0, keepdims=True)
            self.alpha[after, :, lanes] = self.const[after, :, lanes] + top + jnp.log(total) * LOG2E

    def keep(self, k):
        t = self.time(k)
        mine = pl.ds(pl.multiple_of(self.at * 128, 128), 128)
        if k % 2 == 0:
            self.own[t] = self.alpha[t, :, mine]
        else:
            block = self.col[mine, :]
            eye = lax.broadcasted_iota(jnp.int32, (128, 128), 0) == lax.broadcasted_iota(
                jnp.int32, (128, 128), 1
            )
            self.own[t] = jnp.sum(jnp.where(eye, block, 0.0), axis=0, keepdims=True)

    def log_total(self):
        phi = self.alpha[self.time(self.links)] + self.rest[...]
        peak = jnp.max(phi, axis=1, keepdims=True)
        return peak + jnp.log(jnp.sum(jnp.exp2(phi - peak), axis=1, keepdims=True)) * LOG2E

    def loop(self, count, body):
        def turn(i, carry):
            body(i)
            return carry

        lax.fori_loop(0, count, turn, 0)

    def whole(self, action, low=0, high=None):
        for r in range(low, self.tiles if high is None else high):
            action(r)

    def run(self, ready, done):
        half = self.links // 2
        line = self.tiles // 2
        near, far = slice(0, line * 128), slice(line * 128, self.tiles * 128)
        ready(0)
        self.whole(lambda r: self.constants(0, r), high=line)
        self.whole(lambda r: self.prep_even(0, r), high=line)
        self.whole(lambda r: self.constants(1, r), high=line)
        self.whole(lambda r: self.prep_odd(1, r), high=line)
        self.partial(0, near, range(line), True)
        ready("sources")
        self.whole(lambda r: self.constants(0, r), low=line)
        self.whole(lambda r: self.prep_even(0, r), low=line)
        self.partial(0, near, range(line, self.tiles), False)
        ready(1)
        self.whole(lambda r: self.constants(1, r), low=line)
        self.whole(lambda r: self.prep_odd(1, r), low=line)
        self.partial(0, far, range(self.tiles), True)
        for link in range(self.links):
            early = link + 1 < self.links and link >= half - 1
            if early:
                ready(link + 2)
            if link:
                self.message(link, 0)
            if early:
                self.whole(lambda r: self.prep(link + 1, r))
            if link % 2 == 0:
                self.reduce_lanes(0)
            self.keep(link + 1)
            done(link + 1)
            if link + 1 < self.links and not early:
                ready(link + 2)
                self.whole(lambda r: self.prep(link + 1, r))


def chain_kernel(links, tiles, pts, pot, out, *scratch):
    held, *pairs = scratch[:5]
    right, left = pairs[0:2], pairs[2:4]
    alpha, const, rest, col, own, other = scratch[5:11]
    line_send, line_recv, pair_send, pair_recv, core_send, core_recv, end_send, end_recv = scratch[11:19]
    fill, tops, own_pts, own_pot, stage = scratch[19:]
    me = lax.axis_index("tile")
    way = lax.axis_index("link")
    line = tiles // 2
    at, side = me // 2, me % 2
    half = links // 2
    chunks = [(k, 1) for k in range(half + 1)]
    time = lambda k: k + way * (links - 2 * k)
    first = lambda k, count: k + way * (links - 2 * k - count + 1)
    slot = lambda z, y: 2 * z + y
    place = lambda r: slot(r % line, side if r < line else 1 - side)
    ahead = lambda d: slot(lax.rem(at + d, line), side)
    behind = lambda d: lax.rem(at + line - d, line)
    chain = Chain(
        links, tiles, pts.shape[1], held, right, left, alpha, const, rest, col, own, tops, at, place, time
    )

    early = pl.ds(way * half, half + 1)
    mine = [
        pltpu.make_async_copy(pot, own_pot, fill.at[0]),
        pltpu.make_async_copy(pts.at[early], own_pts, fill.at[1]),
    ]
    for copy in mine:
        copy.start()

    barrier = pltpu.get_barrier_semaphore()
    peers = [{"tile": ahead(d)} for d in range(1, line)]
    peers += [{"tile": slot(at, 1 - side)}, {"link": 1 - way}]
    for peer in peers:
        pl.semaphore_signal(barrier, inc=1, device_id=peer)
    for copy in mine:
        copy.wait()
    for j in range(half + 1):
        t = way * half + j
        block = jnp.concatenate([own_pts[j], own_pot[pl.ds(t, 1), :]], axis=0)
        stage[j] = block
        held[t, me] = block
    for buffer in right:
        buffer[192:256, :] = jnp.zeros((64, tiles * 128), jnp.bfloat16)
    pl.semaphore_wait(barrier, len(peers))

    def views(c, origin, source_own):
        k, count = chunks[c]
        span = pl.ds(first(k, count), count)
        part = pl.ds(first(k, count) - way * half, count)
        return (stage.at[part] if source_own else held.at[span, origin]), held.at[span, origin]

    def remote(c, origin, source_own, send, recv, d, device):
        src, dst = views(c, origin, source_own)
        return pltpu.make_async_remote_copy(
            src_ref=src,
            dst_ref=dst,
            send_sem=send.at[c, d],
            recv_sem=recv.at[c, d],
            device_id=device,
        )

    partner = {"tile": slot(at, 1 - side)}
    sent = []

    def to_line(c, d):
        copy = remote(c, me, True, line_send, line_recv, d, {"tile": ahead(d)})
        copy.start()
        sent.append(copy)

    def to_pair(c, d):
        origin = slot(behind(d), side)
        copy = remote(c, origin, d == 0, pair_send, pair_recv, d, partner)
        copy.start()
        sent.append(copy)

    def forward(c):
        for d in range(1, line):
            origin = slot(behind(d), side)
            remote(c, origin, False, line_send, line_recv, d, partner).wait_recv()
            to_pair(c, d)

    def arrive(c):
        for d in range(line):
            origin = slot(behind(d), 1 - side)
            remote(c, origin, False, pair_send, pair_recv, d, partner).wait_recv()

    def across(k):
        t = time(k)
        copy = pltpu.make_async_remote_copy(
            src_ref=held.at[t],
            dst_ref=held.at[t],
            send_sem=core_send.at[k],
            recv_sem=core_recv.at[k],
            device_id={"link": 1 - way},
        )
        copy.start()
        sent.append(copy)

    def from_core(k):
        t = time(links - k)
        pltpu.make_async_remote_copy(
            src_ref=held.at[t],
            dst_ref=held.at[t],
            send_sem=core_send.at[k],
            recv_sem=core_recv.at[k],
            device_id={"link": 1 - way},
        ).wait_recv()

    def rows(which):
        return pl.ds(first(half, half), half) if which == 0 else pl.ds(time(links), 1)

    def ends(which, span):
        return pltpu.make_async_remote_copy(
            src_ref=own.at[span],
            dst_ref=other.at[span],
            send_sem=end_send.at[which],
            recv_sem=end_recv.at[which],
            device_id={"link": 1 - way},
        )

    for c in range(len(chunks)):
        for d in range(line - 1, 0, -1):
            to_line(c, d)
        to_pair(c, 0)

    def ready(k):
        if k == 0:
            for c in range(3):
                forward(c)
        elif k == "sources":
            arrive(0)
            across(0)
        elif k <= half:
            if k + 2 <= half:
                forward(k + 2)
            arrive(k)
            if k < half:
                across(k)
        elif k == half + 1:
            for c in range(half - 1, -1, -1):
                from_core(c)

    def done(k):
        if k == links:
            for which in range(2):
                copy = ends(which, rows(which))
                copy.start()
                sent.append(copy)

    chain.run(ready, done)
    chain.keep(0)
    total = chain.log_total()
    last = [sent.pop(), sent.pop()]
    for copy in sent:
        copy.wait_send()
    ends(0, rows_other(0, links, half, way)).wait_recv()
    ends(1, rows_other(1, links, half, way)).wait_recv()
    lanes = pl.ds(pl.multiple_of(at * 128, 128), 128)
    keep = -math.log(tiles * 128)
    for j in range(half):
        t = 1 + way * half + j
        combined = own[t] + other[t] - const[t, :, lanes]
        out[pl.ds(j, 1), :] = keep - (combined - total) / LOG2E
    for copy in last:
        copy.wait_send()


def rows_other(which, links, half, way):
    back = 1 - way
    if which == 0:
        return pl.ds(half + back * (1 - half), half)
    return pl.ds(links - back * links, 1)


def local_fast(points, potentials):
    times, pcs, cell_dev = points.shape
    links = times - 1
    tiles = lax.axis_size("tile")
    cells = tiles * cell_dev
    vmem = pl.BlockSpec(memory_space=pltpu.VMEM)
    hbm = pl.BlockSpec(memory_space=pltpu.HBM)
    dma = pltpu.SemaphoreType.DMA
    phases = links // 2 + 1
    line = tiles // 2
    return pl.pallas_call(
        functools.partial(chain_kernel, links, tiles),
        out_shape=jax.ShapeDtypeStruct((links // 2, 128), jnp.float32),
        in_specs=[hbm] * 2,
        out_specs=vmem,
        scratch_shapes=[
            pltpu.VMEM((times, tiles, pcs + 1, 128), jnp.float32),
            pltpu.VMEM((256, cells), jnp.bfloat16),
            pltpu.VMEM((256, cells), jnp.bfloat16),
            pltpu.VMEM((cells, 256), jnp.bfloat16),
            pltpu.VMEM((cells, 256), jnp.bfloat16),
            pltpu.VMEM((times, 1, cells), jnp.float32),
            pltpu.VMEM((times, 1, cells), jnp.float32),
            pltpu.VMEM((1, cells), jnp.float32),
            pltpu.VMEM((cells, 128), jnp.float32),
            pltpu.VMEM((times, 1, 128), jnp.float32),
            pltpu.VMEM((times, 1, 128), jnp.float32),
            dma((phases, line)),
            dma((phases, line)),
            dma((phases, line)),
            dma((phases, line)),
            dma((links // 2,)),
            dma((links // 2,)),
            dma((2,)),
            dma((2,)),
            dma((2,)),
            pltpu.VMEM((cells, 128), jnp.float32),
            pltpu.VMEM((links // 2 + 1, pcs, 128), jnp.float32),
            pltpu.VMEM((times, 128), jnp.float32),
            pltpu.VMEM((links // 2 + 1, pcs + 1, 128), jnp.float32),
        ],
        compiler_params=pltpu.CompilerParams(
            vmem_limit_bytes=66900000, collective_id=0, has_side_effects=True
        ),
    )(points, potentials)


def passed_along(block, axis, distance):
    devices = range(lax.axis_size(axis))
    route = [(i - distance, i) for i in devices if i - distance in devices]
    return lax.ppermute(block, axis, route)


def joined(part, axis, combine):
    gathered = jax.tree.map(lambda a: lax.all_gather(a, axis), part)

    def take(source):
        return jax.tree.map(lambda a: lax.dynamic_index_in_dim(a, source, 0, False), gathered)

    return lax.fori_loop(
        1, lax.axis_size(axis), lambda source, state: combine(state, take(source)), take(0)
    )


def pair_scores(source_pts, target_pts, source_msg):
    source_sq = jnp.sum(source_pts * source_pts, axis=0)
    target_sq = jnp.sum(target_pts * target_pts, axis=0)
    inner_prod = lax.dot_general(
        source_pts,
        target_pts,
        (((0,), (0,)), ((), ())),
        precision=lax.Precision.HIGHEST,
        preferred_element_type=jnp.float32,
    )
    pair_cost = source_sq[:, None] + target_sq[None, :] - 2.0 * inner_prod
    return source_msg[:, None] - pair_cost / EPSILON


def combine_lse(left_pair, right_pair):
    peak = jnp.maximum(left_pair[0], right_pair[0])
    return (
        peak,
        left_pair[1] * jnp.exp(left_pair[0] - peak) + right_pair[1] * jnp.exp(right_pair[0] - peak),
    )


def local(points, potentials):
    link_index = lax.axis_index("link")
    link_count = lax.axis_size("link")
    tile_count = lax.axis_size("tile")
    per_link = (points.shape[0] - 1) // link_count
    cell_dev = points.shape[2]
    total_cells = tile_count * cell_dev
    offset_link = link_index * per_link
    local_pts = lax.dynamic_slice_in_dim(points, offset_link, per_link + 1, 0)
    local_pot = lax.dynamic_slice_in_dim(potentials, offset_link, per_link + 1, 0)
    every_pts = lax.all_gather(local_pts, "tile", axis=2, tiled=True)

    def message(source_idx, target_idx, source_msg):
        source_pts = local_pts[source_idx]
        target_pot = local_pot[target_idx]
        target_all = every_pts[target_idx]
        scores = pair_scores(source_pts, target_all, source_msg)
        peak = jnp.max(scores, axis=0)
        partial_lse = peak + jnp.log(jnp.sum(jnp.exp(scores - peak[None, :]), axis=0))
        lse_parts = lax.all_to_all(
            partial_lse.reshape(tile_count, cell_dev),
            "tile",
            split_axis=0,
            concat_axis=0,
            tiled=True,
        )
        peak = jnp.max(lse_parts, axis=0)
        summed = jnp.sum(jnp.exp(lse_parts - peak[None, :]), axis=0)
        return target_pot + peak + jnp.log(summed)

    def sweep(start_msg, forward):
        start_pos = jnp.where(forward, 0, per_link).astype(jnp.int32)
        stored = jnp.zeros((per_link + 1, cell_dev), jnp.float32)
        stored = lax.dynamic_update_slice_in_dim(stored, start_msg[None, :], start_pos, 0)
        current = start_msg
        for link_step in range(per_link):
            source_idx = jnp.where(forward, link_step, per_link - link_step).astype(jnp.int32)
            target_idx = jnp.where(forward, link_step + 1, per_link - 1 - link_step).astype(
                jnp.int32
            )
            current = message(source_idx, target_idx, current)
            stored = lax.dynamic_update_slice_in_dim(stored, current[None, :], target_idx, 0)
        return stored

    first_end = link_index == 0
    early_pass = sweep(local_pot[0], True)
    handed = passed_along(early_pass[per_link], "link", 1)
    forward_msgs = sweep(jnp.where(first_end, local_pot[0], handed), True)
    late_pass = sweep(local_pot[per_link], False)
    handed_back = passed_along(late_pass[0], "link", -1)
    backward_msgs = sweep(jnp.where(first_end, handed_back, local_pot[per_link]), False)
    combined = forward_msgs + backward_msgs - local_pot
    last_row = combined[per_link]
    peak = jnp.max(last_row)
    summed = jnp.sum(jnp.exp(last_row - peak))
    peak, summed = joined((peak, summed), "tile", combine_lse)
    log_total = peak + jnp.log(summed)
    return -math.log(total_cells) - (combined[1:] - log_total)


def fits(mesh, points):
    times, pcs, total = points.shape
    cell_dev = total // (mesh.shape["groups"] * mesh.shape["tile"])
    cells = cell_dev * mesh.shape["tile"]
    held = 2 * cells * cells * 4 + 2 * times * cells * 32 * 4
    return (
        cell_dev == 128
        and pcs < 31
        and times % 2 == 1
        and mesh.shape["tile"] % 2 == 0
        and cells % STRIP == 0
        and mesh.shape["link"] == 2
        and held < 32 * 1024 * 1024
    )


def solution(mesh):
    placed = (P(None, None, ("groups", "tile")), P(None, ("groups", "tile")))

    def whole(points, potentials):
        body = local_fast if fits(mesh, points) else local
        return jax.shard_map(
            body, mesh=mesh, in_specs=placed, out_specs=P("link", ("groups", "tile")), check_vma=False
        )(points, potentials)

    return whole
```

```python
import functools
import math

import jax
import jax.numpy as jnp
from jax import lax
from jax.experimental import pallas as pl
from jax.experimental.pallas import tpu as pltpu
from jax.sharding import PartitionSpec as P

EPSILON = 0.5
LOG2E = math.log2(math.e)
SCALE = 2.0 / EPSILON * LOG2E
STRIP = 1024
ROWS = 8
BLOCK = 32
BAND = 512


def pieces(value):
    high = value.astype(jnp.bfloat16)
    rest = value - high.astype(jnp.float32)
    middle = rest.astype(jnp.bfloat16)
    low = (rest - middle.astype(jnp.float32)).astype(jnp.bfloat16)
    return high, middle, low


def padded(points, extra, slot):
    pad = 32 - points.shape[0]
    row = lax.broadcasted_iota(jnp.int32, (pad, points.shape[1]), 0)
    tail = jnp.where(row == slot, extra, 0.0)
    return jnp.concatenate([points, tail], axis=0)


class Chain:
    def __init__(self, links, tiles, pcs, pts, right, left, alpha, const, rest, col, own, tops, at, place, time):
        self.links, self.tiles = links, tiles
        self.pts, self.pcs = pts, pcs
        self.right, self.left = right, left
        self.alpha, self.const, self.rest = alpha, const, rest
        self.col, self.own, self.tops = col, own, tops
        self.at, self.place, self.time = at, place, time

    def constants(self, k, r):
        t = self.time(k)
        x = self.pts[t, self.place(r), : self.pcs]
        lanes = pl.ds(pl.multiple_of(r * 128, 128), 128)
        square = jnp.sum(x * x, axis=0, keepdims=True)
        pot = self.pts[t, self.place(r), self.pcs :]
        self.const[t, :, lanes] = (pot - (2.0 / EPSILON) * square) * LOG2E
        if k == 0:
            self.alpha[t, :, lanes] = (pot - square / EPSILON) * LOG2E
        if k == self.links:
            self.rest[:, lanes] = square * (LOG2E / EPSILON)

    def prep_even(self, k, r):
        slot = (k // 2) % 2
        x = self.pts[self.time(k), self.place(r), : self.pcs]
        h, m, l = pieces(padded(x, jnp.ones((1, 128), jnp.float32), slot))
        lanes = pl.ds(pl.multiple_of(r * 128, 128), 128)
        self.right[slot][0:192, lanes] = jnp.concatenate([h, h, h, m, l, m], axis=0)

    def prep_odd(self, k, r):
        slot = (k // 2) % 2
        t = self.time(k)
        lanes = pl.ds(pl.multiple_of(r * 128, 128), 128)
        x = self.pts[t, self.place(r), : self.pcs] * SCALE
        h, m, l = pieces(padded(x, self.const[t, :, lanes], slot))
        block = jnp.concatenate([h, m, l, h], axis=0)
        block = block.T
        self.left[slot][lanes, 0:128] = block
        self.left[slot][lanes, 128:256] = block

    def prep(self, link, r):
        self.constants(link + 1, r)
        if link % 2 == 0:
            self.prep_odd(link + 1, r)
        else:
            self.prep_even(link + 1, r)

    def reduce_lanes(self, i):
        for j in range(STRIP // ROWS):
            rows = pl.ds(pl.multiple_of(i * STRIP + j * ROWS, ROWS), ROWS)
            top = self.tops[rows, :]
            peak = jnp.max(top, axis=1, keepdims=True)
            total = jnp.sum(self.col[rows, :] * jnp.exp2(top - peak), axis=1, keepdims=True)
            out = peak + jnp.log(total) * LOG2E
            self.col[rows, :] = jnp.broadcast_to(out, (ROWS, 128))

    def partial(self, link, rows, tiles, first):
        source = self.alpha[self.time(link)]
        lanes = slice(tiles[0] * 128, tiles[-1] * 128 + 128)
        for low in range(rows.start, rows.stop, BAND):
            dots = jnp.dot(
                self.left[(link // 2) % 2][low:low + BAND, :],
                self.right[(link // 2) % 2][:, lanes],
                preferred_element_type=jnp.float32,
            )
            for j in range(0, BAND, ROWS):
                here = slice(low + j, low + j + ROWS)
                s = [
                    dots[j:j + ROWS, n * 128:n * 128 + 128] + source[:, c * 128:c * 128 + 128]
                    for n, c in enumerate(tiles)
                ]
                top = functools.reduce(jnp.maximum, s)
                if not first:
                    old = self.tops[here, :]
                    top = jnp.maximum(top, old)
                total = functools.reduce(jnp.add, [jnp.exp2(a - top) for a in s])
                if not first:
                    total = total + self.col[here, :] * jnp.exp2(old - top)
                self.tops[here, :] = top
                self.col[here, :] = total

    def message(self, link, i):
        after = self.time(link + 1)
        if link % 2 == 0:
            self.partial(link, slice(0, self.tiles * 128), range(self.tiles), True)
        else:
            lanes = pl.ds(pl.multiple_of(i * STRIP, STRIP), STRIP)
            cells = self.col.shape[0]
            step = BLOCK
            peak = total = None
            dots = jnp.dot(self.left[(link // 2) % 2][...], self.right[((link + 1) // 2) % 2][:, lanes], preferred_element_type=jnp.float32)
            for j in range(cells // step):
                rows = slice(j * step, (j + 1) * step)
                source = self.col[rows, :]
                s = dots[rows, :] + jnp.concatenate([source] * (STRIP // 128), axis=1)
                s = s.reshape(step // 8, 8, STRIP)
                top = jnp.max(s, axis=0)
                if peak is None:
                    peak = top
                    total = jnp.sum(jnp.exp2(s - peak[None]), axis=0)
                else:
                    new = jnp.maximum(peak, top)
                    total = total * jnp.exp2(peak - new) + jnp.sum(jnp.exp2(s - new[None]), axis=0)
                    peak = new
            top = jnp.max(peak, axis=0, keepdims=True)
            total = jnp.sum(total * jnp.exp2(peak - top), axis=0, keepdims=True)
            self.alpha[after, :, lanes] = self.const[after, :, lanes] + top + jnp.log(total) * LOG2E

    def keep(self, k):
        t = self.time(k)
        mine = pl.ds(pl.multiple_of(self.at * 128, 128), 128)
        if k % 2 == 0:
            self.own[t] = self.alpha[t, :, mine]
        else:
            block = self.col[mine, :]
            eye = lax.broadcasted_iota(jnp.int32, (128, 128), 0) == lax.broadcasted_iota(
                jnp.int32, (128, 128), 1
            )
            self.own[t] = jnp.sum(jnp.where(eye, block, 0.0), axis=0, keepdims=True)

    def log_total(self):
        phi = self.alpha[self.time(self.links)] + self.rest[...]
        peak = jnp.max(phi, axis=1, keepdims=True)
        return peak + jnp.log(jnp.sum(jnp.exp2(phi - peak), axis=1, keepdims=True)) * LOG2E

    def loop(self, count, body):
        def turn(i, carry):
            body(i)
            return carry

        lax.fori_loop(0, count, turn, 0)

    def whole(self, action, low=0, high=None):
        for r in range(low, self.tiles if high is None else high):
            action(r)

    def run(self, ready, done):
        half = self.links // 2
        line = self.tiles // 2
        near, far = slice(0, line * 128), slice(line * 128, self.tiles * 128)
        ready(0)
        self.whole(lambda r: self.constants(0, r), high=line)
        self.whole(lambda r: self.prep_even(0, r), high=line)
        self.whole(lambda r: self.constants(1, r), high=line)
        self.whole(lambda r: self.prep_odd(1, r), high=line)
        self.partial(0, near, range(line), True)
        ready("sources")
        self.whole(lambda r: self.constants(0, r), low=line)
        self.whole(lambda r: self.prep_even(0, r), low=line)
        self.partial(0, near, range(line, self.tiles), False)
        ready(1)
        self.whole(lambda r: self.constants(1, r), low=line)
        self.whole(lambda r: self.prep_odd(1, r), low=line)
        self.partial(0, far, range(self.tiles), True)
        for link in range(self.links):
            early = link + 1 < self.links and link >= half - 1
            if early:
                ready(link + 2)
            if link:
                self.message(link, 0)
            if early:
                self.whole(lambda r: self.prep(link + 1, r))
            if link % 2 == 0:
                self.reduce_lanes(0)
            self.keep(link + 1)
            done(link + 1)
            if link + 1 < self.links and not early:
                ready(link + 2)
                self.whole(lambda r: self.prep(link + 1, r))


def chain_kernel(links, tiles, pts, pot, out, *scratch):
    held, *pairs = scratch[:5]
    right, left = pairs[0:2], pairs[2:4]
    alpha, const, rest, col, own, other = scratch[5:11]
    line_send, line_recv, pair_send, pair_recv, core_send, core_recv, end_send, end_recv = scratch[11:19]
    fill, tops, own_pts, own_pot, stage = scratch[19:]
    me = lax.axis_index("tile")
    way = lax.axis_index("link")
    line = tiles // 2
    at, side = me // 2, me % 2
    half = links // 2
    chunks = [(k, 1) for k in range(half + 1)]
    time = lambda k: k + way * (links - 2 * k)
    first = lambda k, count: k + way * (links - 2 * k - count + 1)
    slot = lambda z, y: 2 * z + y
    place = lambda r: slot(r % line, side if r < line else 1 - side)
    ahead = lambda d: slot(lax.rem(at + d, line), side)
    behind = lambda d: lax.rem(at + line - d, line)
    chain = Chain(
        links, tiles, pts.shape[1], held, right, left, alpha, const, rest, col, own, tops, at, place, time
    )

    early = pl.ds(way * half, half + 1)
    mine = [
        pltpu.make_async_copy(pot, own_pot, fill.at[0]),
        pltpu.make_async_copy(pts.at[early], own_pts, fill.at[1]),
    ]
    for copy in mine:
        copy.start()

    barrier = pltpu.get_barrier_semaphore()
    peers = [{"tile": ahead(d)} for d in range(1, line)]
    peers += [{"tile": slot(at, 1 - side)}, {"link": 1 - way}]
    for peer in peers:
        pl.semaphore_signal(barrier, inc=1, device_id=peer)
    for copy in mine:
        copy.wait()
    for j in range(half + 1):
        t = way * half + j
        block = jnp.concatenate([own_pts[j], own_pot[pl.ds(t, 1), :]], axis=0)
        stage[j] = block
        held[t, me] = block
    for buffer in right:
        buffer[192:256, :] = jnp.zeros((64, tiles * 128), jnp.bfloat16)
    pl.semaphore_wait(barrier, len(peers))

    def views(c, origin, source_own):
        k, count = chunks[c]
        span = pl.ds(first(k, count), count)
        part = pl.ds(first(k, count) - way * half, count)
        return (stage.at[part] if source_own else held.at[span, origin]), held.at[span, origin]

    def remote(c, origin, source_own, send, recv, d, device):
        src, dst = views(c, origin, source_own)
        return pltpu.make_async_remote_copy(
            src_ref=src,
            dst_ref=dst,
            send_sem=send.at[c, d],
            recv_sem=recv.at[c, d],
            device_id=device,
        )

    partner = {"tile": slot(at, 1 - side)}
    sent = []

    def to_line(c, d):
        copy = remote(c, me, True, line_send, line_recv, d, {"tile": ahead(d)})
        copy.start()
        sent.append(copy)

    def to_pair(c, d):
        origin = slot(behind(d), side)
        copy = remote(c, origin, d == 0, pair_send, pair_recv, d, partner)
        copy.start()
        sent.append(copy)

    def forward(c):
        for d in range(1, line):
            origin = slot(behind(d), side)
            remote(c, origin, False, line_send, line_recv, d, partner).wait_recv()
            to_pair(c, d)

    def arrive(c):
        for d in range(line):
            origin = slot(behind(d), 1 - side)
            remote(c, origin, False, pair_send, pair_recv, d, partner).wait_recv()

    def across(k):
        t = time(k)
        copy = pltpu.make_async_remote_copy(
            src_ref=held.at[t],
            dst_ref=held.at[t],
            send_sem=core_send.at[k],
            recv_sem=core_recv.at[k],
            device_id={"link": 1 - way},
        )
        copy.start()
        sent.append(copy)

    def from_core(k):
        t = time(links - k)
        pltpu.make_async_remote_copy(
            src_ref=held.at[t],
            dst_ref=held.at[t],
            send_sem=core_send.at[k],
            recv_sem=core_recv.at[k],
            device_id={"link": 1 - way},
        ).wait_recv()

    def rows(which):
        return pl.ds(first(half, half), half) if which == 0 else pl.ds(time(links), 1)

    def ends(which, span):
        return pltpu.make_async_remote_copy(
            src_ref=own.at[span],
            dst_ref=other.at[span],
            send_sem=end_send.at[which],
            recv_sem=end_recv.at[which],
            device_id={"link": 1 - way},
        )

    for c in range(len(chunks)):
        for d in range(line - 1, 0, -1):
            to_line(c, d)
        to_pair(c, 0)

    def ready(k):
        if k == 0:
            for c in range(3):
                forward(c)
        elif k == "sources":
            arrive(0)
            across(0)
        elif k <= half:
            if k + 2 <= half:
                forward(k + 2)
            arrive(k)
            if k < half:
                across(k)
        elif k == half + 1:
            for c in range(half - 1, -1, -1):
                from_core(c)

    def done(k):
        if k == links:
            for which in range(2):
                copy = ends(which, rows(which))
                copy.start()
                sent.append(copy)

    chain.run(ready, done)
    chain.keep(0)
    total = chain.log_total()
    last = [sent.pop(), sent.pop()]
    for copy in sent:
        copy.wait_send()
    ends(0, rows_other(0, links, half, way)).wait_recv()
    ends(1, rows_other(1, links, half, way)).wait_recv()
    lanes = pl.ds(pl.multiple_of(at * 128, 128), 128)
    keep = -math.log(tiles * 128)
    for j in range(half):
        t = 1 + way * half + j
        combined = own[t] + other[t] - const[t, :, lanes]
        out[pl.ds(j, 1), :] = keep - (combined - total) / LOG2E
    for copy in last:
        copy.wait_send()


def rows_other(which, links, half, way):
    back = 1 - way
    if which == 0:
        return pl.ds(half + back * (1 - half), half)
    return pl.ds(links - back * links, 1)


def local_fast(points, potentials):
    times, pcs, cell_dev = points.shape
    links = times - 1
    tiles = lax.axis_size("tile")
    cells = tiles * cell_dev
    vmem = pl.BlockSpec(memory_space=pltpu.VMEM)
    hbm = pl.BlockSpec(memory_space=pltpu.HBM)
    dma = pltpu.SemaphoreType.DMA
    phases = links // 2 + 1
    line = tiles // 2
    return pl.pallas_call(
        functools.partial(chain_kernel, links, tiles),
        out_shape=jax.ShapeDtypeStruct((links // 2, 128), jnp.float32),
        in_specs=[hbm] * 2,
        out_specs=vmem,
        scratch_shapes=[
            pltpu.VMEM((times, tiles, pcs + 1, 128), jnp.float32),
            pltpu.VMEM((256, cells), jnp.bfloat16),
            pltpu.VMEM((256, cells), jnp.bfloat16),
            pltpu.VMEM((cells, 256), jnp.bfloat16),
            pltpu.VMEM((cells, 256), jnp.bfloat16),
            pltpu.VMEM((times, 1, cells), jnp.float32),
            pltpu.VMEM((times, 1, cells), jnp.float32),
            pltpu.VMEM((1, cells), jnp.float32),
            pltpu.VMEM((cells, 128), jnp.float32),
            pltpu.VMEM((times, 1, 128), jnp.float32),
            pltpu.VMEM((times, 1, 128), jnp.float32),
            dma((phases, line)),
            dma((phases, line)),
            dma((phases, line)),
            dma((phases, line)),
            dma((links // 2,)),
            dma((links // 2,)),
            dma((2,)),
            dma((2,)),
            dma((2,)),
            pltpu.VMEM((cells, 128), jnp.float32),
            pltpu.VMEM((links // 2 + 1, pcs, 128), jnp.float32),
            pltpu.VMEM((times, 128), jnp.float32),
            pltpu.VMEM((links // 2 + 1, pcs + 1, 128), jnp.float32),
        ],
        compiler_params=pltpu.CompilerParams(
            vmem_limit_bytes=66900000, collective_id=0, has_side_effects=True
        ),
    )(points, potentials)


def passed_along(block, axis, distance):
    devices = range(lax.axis_size(axis))
    route = [(i - distance, i) for i in devices if i - distance in devices]
    return lax.ppermute(block, axis, route)


def joined(part, axis, combine):
    gathered = jax.tree.map(lambda a: lax.all_gather(a, axis), part)

    def take(source):
        return jax.tree.map(lambda a: lax.dynamic_index_in_dim(a, source, 0, False), gathered)

    return lax.fori_loop(
        1, lax.axis_size(axis), lambda source, state: combine(state, take(source)), take(0)
    )


def pair_scores(source_pts, target_pts, source_msg):
    source_sq = jnp.sum(source_pts * source_pts, axis=0)
    target_sq = jnp.sum(target_pts * target_pts, axis=0)
    inner_prod = lax.dot_general(
        source_pts,
        target_pts,
        (((0,), (0,)), ((), ())),
        precision=lax.Precision.HIGHEST,
        preferred_element_type=jnp.float32,
    )
    pair_cost = source_sq[:, None] + target_sq[None, :] - 2.0 * inner_prod
    return source_msg[:, None] - pair_cost / EPSILON


def combine_lse(left_pair, right_pair):
    peak = jnp.maximum(left_pair[0], right_pair[0])
    return (
        peak,
        left_pair[1] * jnp.exp(left_pair[0] - peak) + right_pair[1] * jnp.exp(right_pair[0] - peak),
    )


def local(points, potentials):
    link_index = lax.axis_index("link")
    link_count = lax.axis_size("link")
    tile_count = lax.axis_size("tile")
    per_link = (points.shape[0] - 1) // link_count
    cell_dev = points.shape[2]
    total_cells = tile_count * cell_dev
    offset_link = link_index * per_link
    local_pts = lax.dynamic_slice_in_dim(points, offset_link, per_link + 1, 0)
    local_pot = lax.dynamic_slice_in_dim(potentials, offset_link, per_link + 1, 0)
    every_pts = lax.all_gather(local_pts, "tile", axis=2, tiled=True)

    def message(source_idx, target_idx, source_msg):
        source_pts = local_pts[source_idx]
        target_pot = local_pot[target_idx]
        target_all = every_pts[target_idx]
        scores = pair_scores(source_pts, target_all, source_msg)
        peak = jnp.max(scores, axis=0)
        partial_lse = peak + jnp.log(jnp.sum(jnp.exp(scores - peak[None, :]), axis=0))
        lse_parts = lax.all_to_all(
            partial_lse.reshape(tile_count, cell_dev),
            "tile",
            split_axis=0,
            concat_axis=0,
            tiled=True,
        )
        peak = jnp.max(lse_parts, axis=0)
        summed = jnp.sum(jnp.exp(lse_parts - peak[None, :]), axis=0)
        return target_pot + peak + jnp.log(summed)

    def sweep(start_msg, forward):
        start_pos = jnp.where(forward, 0, per_link).astype(jnp.int32)
        stored = jnp.zeros((per_link + 1, cell_dev), jnp.float32)
        stored = lax.dynamic_update_slice_in_dim(stored, start_msg[None, :], start_pos, 0)
        current = start_msg
        for link_step in range(per_link):
            source_idx = jnp.where(forward, link_step, per_link - link_step).astype(jnp.int32)
            target_idx = jnp.where(forward, link_step + 1, per_link - 1 - link_step).astype(
                jnp.int32
            )
            current = message(source_idx, target_idx, current)
            stored = lax.dynamic_update_slice_in_dim(stored, current[None, :], target_idx, 0)
        return stored

    first_end = link_index == 0
    early_pass = sweep(local_pot[0], True)
    handed = passed_along(early_pass[per_link], "link", 1)
    forward_msgs = sweep(jnp.where(first_end, local_pot[0], handed), True)
    late_pass = sweep(local_pot[per_link], False)
    handed_back = passed_along(late_pass[0], "link", -1)
    backward_msgs = sweep(jnp.where(first_end, handed_back, local_pot[per_link]), False)
    combined = forward_msgs + backward_msgs - local_pot
    last_row = combined[per_link]
    peak = jnp.max(last_row)
    summed = jnp.sum(jnp.exp(last_row - peak))
    peak, summed = joined((peak, summed), "tile", combine_lse)
    log_total = peak + jnp.log(summed)
    return -math.log(total_cells) - (combined[1:] - log_total)


def fits(mesh, points):
    times, pcs, total = points.shape
    cell_dev = total // (mesh.shape["groups"] * mesh.shape["tile"])
    cells = cell_dev * mesh.shape["tile"]
    held = 2 * cells * cells * 4 + 2 * times * cells * 32 * 4
    return (
        cell_dev == 128
        and pcs < 31
        and times % 2 == 1
        and mesh.shape["tile"] % 2 == 0
        and cells % STRIP == 0
        and mesh.shape["link"] == 2
        and held < 32 * 1024 * 1024
    )


def solution(mesh):
    placed = (P(None, None, ("groups", "tile")), P(None, ("groups", "tile")))

    def whole(points, potentials):
        body = local_fast if fits(mesh, points) else local
        return jax.shard_map(
            body, mesh=mesh, in_specs=placed, out_specs=P("link", ("groups", "tile")), check_vma=False
        )(points, potentials)

    return whole
```

```python
import functools
import math

import jax
import jax.numpy as jnp
from jax import lax
from jax.experimental import pallas as pl
from jax.experimental.pallas import tpu as pltpu
from jax.sharding import PartitionSpec as P

EPSILON = 0.5
LOG2E = math.log2(math.e)
SCALE = 2.0 / EPSILON * LOG2E
STRIP = 1024
ROWS = 8
BLOCK = 32
BAND = 512


def pieces(value):
    high = value.astype(jnp.bfloat16)
    rest = value - high.astype(jnp.float32)
    middle = rest.astype(jnp.bfloat16)
    low = (rest - middle.astype(jnp.float32)).astype(jnp.bfloat16)
    return high, middle, low


def padded(points, extra, slot):
    pad = 32 - points.shape[0]
    row = lax.broadcasted_iota(jnp.int32, (pad, points.shape[1]), 0)
    tail = jnp.where(row == slot, extra, 0.0)
    return jnp.concatenate([points, tail], axis=0)


class Chain:
    def __init__(self, links, tiles, pcs, pts, right, left, alpha, const, rest, col, own, tops, at, place, time):
        self.links, self.tiles = links, tiles
        self.pts, self.pcs = pts, pcs
        self.right, self.left = right, left
        self.alpha, self.const, self.rest = alpha, const, rest
        self.col, self.own, self.tops = col, own, tops
        self.at, self.place, self.time = at, place, time

    def constants(self, k, r):
        t = self.time(k)
        x = self.pts[t, self.place(r), : self.pcs]
        lanes = pl.ds(pl.multiple_of(r * 128, 128), 128)
        square = jnp.sum(x * x, axis=0, keepdims=True)
        pot = self.pts[t, self.place(r), self.pcs :]
        self.const[t, :, lanes] = (pot - (2.0 / EPSILON) * square) * LOG2E
        if k == 0:
            self.alpha[t, :, lanes] = (pot - square / EPSILON) * LOG2E
        if k == self.links:
            self.rest[:, lanes] = square * (LOG2E / EPSILON)

    def prep_even(self, k, r):
        slot = (k // 2) % 2
        x = self.pts[self.time(k), self.place(r), : self.pcs]
        h, m, l = pieces(padded(x, jnp.ones((1, 128), jnp.float32), slot))
        lanes = pl.ds(pl.multiple_of(r * 128, 128), 128)
        self.right[slot][0:192, lanes] = jnp.concatenate([h, h, h, m, l, m], axis=0)

    def prep_odd(self, k, r):
        slot = (k // 2) % 2
        t = self.time(k)
        lanes = pl.ds(pl.multiple_of(r * 128, 128), 128)
        x = self.pts[t, self.place(r), : self.pcs] * SCALE
        h, m, l = pieces(padded(x, self.const[t, :, lanes], slot))
        block = jnp.concatenate([h, m, l, h], axis=0)
        block = block.T
        self.left[slot][lanes, 0:128] = block
        self.left[slot][lanes, 128:256] = block

    def prep(self, link, r):
        self.constants(link + 1, r)
        if link % 2 == 0:
            self.prep_odd(link + 1, r)
        else:
            self.prep_even(link + 1, r)

    def reduce_lanes(self, i):
        for j in range(STRIP // ROWS):
            rows = pl.ds(pl.multiple_of(i * STRIP + j * ROWS, ROWS), ROWS)
            top = self.tops[rows, :]
            peak = jnp.max(top, axis=1, keepdims=True)
            total = jnp.sum(self.col[rows, :] * jnp.exp2(top - peak), axis=1, keepdims=True)
            out = peak + jnp.log(total) * LOG2E
            self.col[rows, :] = jnp.broadcast_to(out, (ROWS, 128))

    def partial(self, link, rows, tiles, first):
        source = self.alpha[self.time(link)]
        lanes = slice(tiles[0] * 128, tiles[-1] * 128 + 128)
        for low in range(rows.start, rows.stop, BAND):
            dots = jnp.dot(
                self.left[(link // 2) % 2][low:low + BAND, :],
                self.right[(link // 2) % 2][:, lanes],
                preferred_element_type=jnp.float32,
            )
            for j in range(0, BAND, ROWS):
                here = slice(low + j, low + j + ROWS)
                s = [
                    dots[j:j + ROWS, n * 128:n * 128 + 128] + source[:, c * 128:c * 128 + 128]
                    for n, c in enumerate(tiles)
                ]
                top = functools.reduce(jnp.maximum, s)
                if not first:
                    old = self.tops[here, :]
                    top = jnp.maximum(top, old)
                total = functools.reduce(jnp.add, [jnp.exp2(a - top) for a in s])
                if not first:
                    total = total + self.col[here, :] * jnp.exp2(old - top)
                self.tops[here, :] = top
                self.col[here, :] = total

    def message(self, link, i):
        after = self.time(link + 1)
        if link % 2 == 0:
            self.partial(link, slice(0, self.tiles * 128), range(self.tiles), True)
        else:
            lanes = pl.ds(pl.multiple_of(i * STRIP, STRIP), STRIP)
            cells = self.col.shape[0]
            step = BLOCK
            peak = total = None
            dots = jnp.dot(self.left[(link // 2) % 2][...], self.right[((link + 1) // 2) % 2][:, lanes], preferred_element_type=jnp.float32)
            for j in range(cells // step):
                rows = slice(j * step, (j + 1) * step)
                source = self.col[rows, :]
                s = dots[rows, :] + jnp.concatenate([source] * (STRIP // 128), axis=1)
                s = s.reshape(step // 8, 8, STRIP)
                top = jnp.max(s, axis=0)
                if peak is None:
                    peak = top
                    total = jnp.sum(jnp.exp2(s - peak[None]), axis=0)
                else:
                    new = jnp.maximum(peak, top)
                    total = total * jnp.exp2(peak - new) + jnp.sum(jnp.exp2(s - new[None]), axis=0)
                    peak = new
            top = jnp.max(peak, axis=0, keepdims=True)
            total = jnp.sum(total * jnp.exp2(peak - top), axis=0, keepdims=True)
            self.alpha[after, :, lanes] = self.const[after, :, lanes] + top + jnp.log(total) * LOG2E

    def keep(self, k):
        t = self.time(k)
        mine = pl.ds(pl.multiple_of(self.at * 128, 128), 128)
        if k % 2 == 0:
            self.own[t] = self.alpha[t, :, mine]
        else:
            block = self.col[mine, :]
            eye = lax.broadcasted_iota(jnp.int32, (128, 128), 0) == lax.broadcasted_iota(
                jnp.int32, (128, 128), 1
            )
            self.own[t] = jnp.sum(jnp.where(eye, block, 0.0), axis=0, keepdims=True)

    def log_total(self):
        phi = self.alpha[self.time(self.links)] + self.rest[...]
        peak = jnp.max(phi, axis=1, keepdims=True)
        return peak + jnp.log(jnp.sum(jnp.exp2(phi - peak), axis=1, keepdims=True)) * LOG2E

    def loop(self, count, body):
        def turn(i, carry):
            body(i)
            return carry

        lax.fori_loop(0, count, turn, 0)

    def whole(self, action, low=0, high=None):
        for r in range(low, self.tiles if high is None else high):
            action(r)

    def run(self, ready, done):
        half = self.links // 2
        line = self.tiles // 2
        near, far = slice(0, line * 128), slice(line * 128, self.tiles * 128)
        ready(0)
        self.whole(lambda r: self.constants(0, r), high=line)
        self.whole(lambda r: self.prep_even(0, r), high=line)
        self.whole(lambda r: self.constants(1, r), high=line)
        self.whole(lambda r: self.prep_odd(1, r), high=line)
        self.partial(0, near, range(line), True)
        ready("sources")
        self.whole(lambda r: self.constants(0, r), low=line)
        self.whole(lambda r: self.prep_even(0, r), low=line)
        self.partial(0, near, range(line, self.tiles), False)
        ready(1)
        self.whole(lambda r: self.constants(1, r), low=line)
        self.whole(lambda r: self.prep_odd(1, r), low=line)
        self.partial(0, far, range(self.tiles), True)
        for link in range(self.links):
            early = link + 1 < self.links and link >= half - 1
            if early:
                ready(link + 2)
            if link:
                self.message(link, 0)
            if early:
                self.whole(lambda r: self.prep(link + 1, r))
            if link % 2 == 0:
                self.reduce_lanes(0)
            self.keep(link + 1)
            done(link + 1)
            if link + 1 < self.links and not early:
                ready(link + 2)
                self.whole(lambda r: self.prep(link + 1, r))


def chain_kernel(links, tiles, pts, pot, out, *scratch):
    held, *pairs = scratch[:5]
    right, left = pairs[0:2], pairs[2:4]
    alpha, const, rest, col, own, other = scratch[5:11]
    block_send, line_recv, pair_recv, core_send, core_recv, end_send, end_recv = scratch[11:18]
    fill, tops, own_pts, own_pot, stage = scratch[18:]
    me = lax.axis_index("tile")
    way = lax.axis_index("link")
    line = tiles // 2
    at, side = me // 2, me % 2
    half = links // 2
    chunks = [(k, 1) for k in range(half + 1)]
    time = lambda k: k + way * (links - 2 * k)
    first = lambda k, count: k + way * (links - 2 * k - count + 1)
    slot = lambda z, y: 2 * z + y
    place = lambda r: slot(r % line, side if r < line else 1 - side)
    ahead = lambda d: slot(lax.rem(at + d, line), side)
    behind = lambda d: lax.rem(at + line - d, line)
    chain = Chain(
        links, tiles, pts.shape[1], held, right, left, alpha, const, rest, col, own, tops, at, place, time
    )

    early = pl.ds(way * half, half + 1)
    mine = [
        pltpu.make_async_copy(pot, own_pot, fill.at[0]),
        pltpu.make_async_copy(pts.at[early], own_pts, fill.at[1]),
    ]
    for copy in mine:
        copy.start()

    barrier = pltpu.get_barrier_semaphore()
    peers = [{"tile": ahead(d)} for d in range(1, line)]
    peers += [{"tile": slot(at, 1 - side)}, {"link": 1 - way}]
    for peer in peers:
        pl.semaphore_signal(barrier, inc=1, device_id=peer)
    for copy in mine:
        copy.wait()
    for j in range(half + 1):
        t = way * half + j
        block = jnp.concatenate([own_pts[j], own_pot[pl.ds(t, 1), :]], axis=0)
        stage[j] = block
        held[t, me] = block
    for buffer in right:
        buffer[192:256, :] = jnp.zeros((64, tiles * 128), jnp.bfloat16)
    pl.semaphore_wait(barrier, len(peers))

    def views(c, origin, source_own):
        k, count = chunks[c]
        span = pl.ds(first(k, count), count)
        part = pl.ds(first(k, count) - way * half, count)
        return (stage.at[part] if source_own else held.at[span, origin]), held.at[span, origin]

    def remote(c, origin, source_own, recv, device):
        src, dst = views(c, origin, source_own)
        return pltpu.make_async_remote_copy(
            src_ref=src,
            dst_ref=dst,
            send_sem=block_send.at[0],
            recv_sem=recv,
            device_id=device,
        )

    partner = {"tile": slot(at, 1 - side)}
    sent = []

    def all_of(span, send, recv, device):
        return pltpu.make_async_remote_copy(
            src_ref=span, dst_ref=span, send_sem=send, recv_sem=recv, device_id=device
        )

    def to_line(c, d):
        remote(c, me, True, line_recv.at[c, d - 1], {"tile": ahead(d)}).start()

    def to_pair(c, d):
        origin = slot(behind(d), side)
        remote(c, origin, d == 0, pair_recv.at[c], partner).start()

    def forward(c):
        for d in range(1, line):
            origin = slot(behind(d), side)
            remote(c, origin, False, line_recv.at[c, d - 1], partner).wait_recv()
            to_pair(c, d)

    def arrive(c):
        span = held.at[time(chunks[c][0]), pl.ds(0, line)]
        all_of(span, block_send.at[0], pair_recv.at[c], partner).wait_recv()

    def across(k):
        t = time(k)
        copy = pltpu.make_async_remote_copy(
            src_ref=held.at[t],
            dst_ref=held.at[t],
            send_sem=core_send.at[0],
            recv_sem=core_recv.at[k],
            device_id={"link": 1 - way},
        )
        copy.start()

    def from_core(k):
        t = time(links - k)
        pltpu.make_async_remote_copy(
            src_ref=held.at[t],
            dst_ref=held.at[t],
            send_sem=core_send.at[0],
            recv_sem=core_recv.at[k],
            device_id={"link": 1 - way},
        ).wait_recv()

    def rows(which):
        return pl.ds(first(half, half), half) if which == 0 else pl.ds(time(links), 1)

    def ends(which, span):
        return pltpu.make_async_remote_copy(
            src_ref=own.at[span],
            dst_ref=other.at[span],
            send_sem=end_send.at[which],
            recv_sem=end_recv.at[which],
            device_id={"link": 1 - way},
        )

    for c in range(len(chunks)):
        for d in range(line - 1, 0, -1):
            to_line(c, d)
        to_pair(c, 0)

    def ready(k):
        if k == 0:
            for c in range(3):
                forward(c)
        elif k == "sources":
            arrive(0)
            across(0)
        elif k <= half:
            if k + 2 <= half:
                forward(k + 2)
            arrive(k)
            if k < half:
                across(k)
        elif k == half + 1:
            for c in range(half - 1, -1, -1):
                from_core(c)

    def done(k):
        if k == links:
            for which in range(2):
                copy = ends(which, rows(which))
                copy.start()
                sent.append(copy)

    chain.run(ready, done)
    chain.keep(0)
    tops[0:1, :] = jnp.broadcast_to(chain.log_total(), (1, 128))
    lanes = pl.ds(pl.multiple_of(at * 128, 128), 128)
    for j in range(half):
        t = 1 + way * half + j
        tops[pl.ds(8 + j, 1), :] = own[t] - const[t, :, lanes]
    blocks = held.at[pl.ds(0, half + 1), pl.ds(0, 2 * line - 1)]
    all_of(blocks, block_send.at[0], pair_recv.at[0], partner).wait_send()
    all_of(held.at[pl.ds(0, half)], core_send.at[0], core_recv.at[0], {"link": 1 - way}).wait_send()
    ends(0, rows_other(0, links, half, way)).wait_recv()
    ends(1, rows_other(1, links, half, way)).wait_recv()
    keep = -math.log(tiles * 128)
    total = tops[0:1, :]
    for j in range(half):
        t = 1 + way * half + j
        combined = other[t] + tops[8 + j:9 + j, :]
        out[pl.ds(j, 1), :] = keep - (combined - total) / LOG2E
    for copy in sent:
        copy.wait_send()


def rows_other(which, links, half, way):
    back = 1 - way
    if which == 0:
        return pl.ds(half + back * (1 - half), half)
    return pl.ds(links - back * links, 1)


def local_fast(points, potentials):
    times, pcs, cell_dev = points.shape
    links = times - 1
    tiles = lax.axis_size("tile")
    cells = tiles * cell_dev
    vmem = pl.BlockSpec(memory_space=pltpu.VMEM)
    hbm = pl.BlockSpec(memory_space=pltpu.HBM)
    dma = pltpu.SemaphoreType.DMA
    phases = links // 2 + 1
    line = tiles // 2
    return pl.pallas_call(
        functools.partial(chain_kernel, links, tiles),
        out_shape=jax.ShapeDtypeStruct((links // 2, 128), jnp.float32),
        in_specs=[hbm] * 2,
        out_specs=vmem,
        scratch_shapes=[
            pltpu.VMEM((times, tiles, pcs + 1, 128), jnp.float32),
            pltpu.VMEM((256, cells), jnp.bfloat16),
            pltpu.VMEM((256, cells), jnp.bfloat16),
            pltpu.VMEM((cells, 256), jnp.bfloat16),
            pltpu.VMEM((cells, 256), jnp.bfloat16),
            pltpu.VMEM((times, 1, cells), jnp.float32),
            pltpu.VMEM((times, 1, cells), jnp.float32),
            pltpu.VMEM((1, cells), jnp.float32),
            pltpu.VMEM((cells, 128), jnp.float32),
            pltpu.VMEM((times, 1, 128), jnp.float32),
            pltpu.VMEM((times, 1, 128), jnp.float32),
            dma((1,)),
            dma((phases, line - 1)),
            dma((phases,)),
            dma((1,)),
            dma((links // 2,)),
            dma((2,)),
            dma((2,)),
            dma((2,)),
            pltpu.VMEM((cells, 128), jnp.float32),
            pltpu.VMEM((links // 2 + 1, pcs, 128), jnp.float32),
            pltpu.VMEM((times, 128), jnp.float32),
            pltpu.VMEM((links // 2 + 1, pcs + 1, 128), jnp.float32),
        ],
        compiler_params=pltpu.CompilerParams(
            vmem_limit_bytes=66900000, collective_id=0, has_side_effects=True
        ),
    )(points, potentials)


def passed_along(block, axis, distance):
    devices = range(lax.axis_size(axis))
    route = [(i - distance, i) for i in devices if i - distance in devices]
    return lax.ppermute(block, axis, route)


def joined(part, axis, combine):
    gathered = jax.tree.map(lambda a: lax.all_gather(a, axis), part)

    def take(source):
        return jax.tree.map(lambda a: lax.dynamic_index_in_dim(a, source, 0, False), gathered)

    return lax.fori_loop(
        1, lax.axis_size(axis), lambda source, state: combine(state, take(source)), take(0)
    )


def pair_scores(source_pts, target_pts, source_msg):
    source_sq = jnp.sum(source_pts * source_pts, axis=0)
    target_sq = jnp.sum(target_pts * target_pts, axis=0)
    inner_prod = lax.dot_general(
        source_pts,
        target_pts,
        (((0,), (0,)), ((), ())),
        precision=lax.Precision.HIGHEST,
        preferred_element_type=jnp.float32,
    )
    pair_cost = source_sq[:, None] + target_sq[None, :] - 2.0 * inner_prod
    return source_msg[:, None] - pair_cost / EPSILON


def combine_lse(left_pair, right_pair):
    peak = jnp.maximum(left_pair[0], right_pair[0])
    return (
        peak,
        left_pair[1] * jnp.exp(left_pair[0] - peak) + right_pair[1] * jnp.exp(right_pair[0] - peak),
    )


def local(points, potentials):
    link_index = lax.axis_index("link")
    link_count = lax.axis_size("link")
    tile_count = lax.axis_size("tile")
    per_link = (points.shape[0] - 1) // link_count
    cell_dev = points.shape[2]
    total_cells = tile_count * cell_dev
    offset_link = link_index * per_link
    local_pts = lax.dynamic_slice_in_dim(points, offset_link, per_link + 1, 0)
    local_pot = lax.dynamic_slice_in_dim(potentials, offset_link, per_link + 1, 0)
    every_pts = lax.all_gather(local_pts, "tile", axis=2, tiled=True)

    def message(source_idx, target_idx, source_msg):
        source_pts = local_pts[source_idx]
        target_pot = local_pot[target_idx]
        target_all = every_pts[target_idx]
        scores = pair_scores(source_pts, target_all, source_msg)
        peak = jnp.max(scores, axis=0)
        partial_lse = peak + jnp.log(jnp.sum(jnp.exp(scores - peak[None, :]), axis=0))
        lse_parts = lax.all_to_all(
            partial_lse.reshape(tile_count, cell_dev),
            "tile",
            split_axis=0,
            concat_axis=0,
            tiled=True,
        )
        peak = jnp.max(lse_parts, axis=0)
        summed = jnp.sum(jnp.exp(lse_parts - peak[None, :]), axis=0)
        return target_pot + peak + jnp.log(summed)

    def sweep(start_msg, forward):
        start_pos = jnp.where(forward, 0, per_link).astype(jnp.int32)
        stored = jnp.zeros((per_link + 1, cell_dev), jnp.float32)
        stored = lax.dynamic_update_slice_in_dim(stored, start_msg[None, :], start_pos, 0)
        current = start_msg
        for link_step in range(per_link):
            source_idx = jnp.where(forward, link_step, per_link - link_step).astype(jnp.int32)
            target_idx = jnp.where(forward, link_step + 1, per_link - 1 - link_step).astype(
                jnp.int32
            )
            current = message(source_idx, target_idx, current)
            stored = lax.dynamic_update_slice_in_dim(stored, current[None, :], target_idx, 0)
        return stored

    first_end = link_index == 0
    early_pass = sweep(local_pot[0], True)
    handed = passed_along(early_pass[per_link], "link", 1)
    forward_msgs = sweep(jnp.where(first_end, local_pot[0], handed), True)
    late_pass = sweep(local_pot[per_link], False)
    handed_back = passed_along(late_pass[0], "link", -1)
    backward_msgs = sweep(jnp.where(first_end, handed_back, local_pot[per_link]), False)
    combined = forward_msgs + backward_msgs - local_pot
    last_row = combined[per_link]
    peak = jnp.max(last_row)
    summed = jnp.sum(jnp.exp(last_row - peak))
    peak, summed = joined((peak, summed), "tile", combine_lse)
    log_total = peak + jnp.log(summed)
    return -math.log(total_cells) - (combined[1:] - log_total)


def fits(mesh, points):
    times, pcs, total = points.shape
    cell_dev = total // (mesh.shape["groups"] * mesh.shape["tile"])
    cells = cell_dev * mesh.shape["tile"]
    held = 2 * cells * cells * 4 + 2 * times * cells * 32 * 4
    return (
        cell_dev == 128
        and pcs < 31
        and times % 2 == 1
        and mesh.shape["tile"] % 2 == 0
        and cells % STRIP == 0
        and mesh.shape["link"] == 2
        and held < 32 * 1024 * 1024
    )


def solution(mesh):
    placed = (P(None, None, ("groups", "tile")), P(None, ("groups", "tile")))

    def whole(points, potentials):
        body = local_fast if fits(mesh, points) else local
        return jax.shard_map(
            body, mesh=mesh, in_specs=placed, out_specs=P("link", ("groups", "tile")), check_vma=False
        )(points, potentials)

    return whole
```

```python
import functools
import math

import jax
import jax.numpy as jnp
from jax import lax
from jax.experimental import pallas as pl
from jax.experimental.pallas import tpu as pltpu
from jax.sharding import PartitionSpec as P

EPSILON = 0.5
LOG2E = math.log2(math.e)
SCALE = 2.0 / EPSILON * LOG2E
STRIP = 1024
ROWS = 8
BLOCK = 32
BAND = 512


def pieces(value):
    high = value.astype(jnp.bfloat16)
    rest = value - high.astype(jnp.float32)
    middle = rest.astype(jnp.bfloat16)
    low = (rest - middle.astype(jnp.float32)).astype(jnp.bfloat16)
    return high, middle, low


def padded(points, extra, slot):
    pad = 32 - points.shape[0]
    row = lax.broadcasted_iota(jnp.int32, (pad, points.shape[1]), 0)
    tail = jnp.where(row == slot, extra, 0.0)
    return jnp.concatenate([points, tail], axis=0)


class Chain:
    def __init__(self, links, tiles, pcs, pts, right, left, alpha, const, rest, col, own, tops, at, place, time):
        self.links, self.tiles = links, tiles
        self.pts, self.pcs = pts, pcs
        self.right, self.left = right, left
        self.alpha, self.const, self.rest = alpha, const, rest
        self.col, self.own, self.tops = col, own, tops
        self.at, self.place, self.time = at, place, time

    def constants(self, k, r):
        t = self.time(k)
        x = self.pts[t, self.place(r), : self.pcs]
        lanes = pl.ds(pl.multiple_of(r * 128, 128), 128)
        square = jnp.sum(x * x, axis=0, keepdims=True)
        pot = self.pts[t, self.place(r), self.pcs :]
        self.const[t, :, lanes] = (pot - (2.0 / EPSILON) * square) * LOG2E
        if k == 0:
            self.alpha[t, :, lanes] = (pot - square / EPSILON) * LOG2E
        if k == self.links:
            self.rest[:, lanes] = square * (LOG2E / EPSILON)

    def prep_even(self, k, r):
        slot = (k // 2) % 2
        x = self.pts[self.time(k), self.place(r), : self.pcs]
        h, m, l = pieces(padded(x, jnp.ones((1, 128), jnp.float32), slot))
        lanes = pl.ds(pl.multiple_of(r * 128, 128), 128)
        self.right[slot][0:192, lanes] = jnp.concatenate([h, h, h, m, l, m], axis=0)

    def prep_odd(self, k, r):
        slot = (k // 2) % 2
        t = self.time(k)
        lanes = pl.ds(pl.multiple_of(r * 128, 128), 128)
        x = self.pts[t, self.place(r), : self.pcs] * SCALE
        h, m, l = pieces(padded(x, self.const[t, :, lanes], slot))
        block = jnp.concatenate([h, m, l, h], axis=0)
        block = block.T
        self.left[slot][lanes, 0:128] = block
        self.left[slot][lanes, 128:256] = block

    def prep(self, link, r):
        self.constants(link + 1, r)
        if link % 2 == 0:
            self.prep_odd(link + 1, r)
        else:
            self.prep_even(link + 1, r)

    def reduce_lanes(self, i):
        for j in range(STRIP // ROWS):
            rows = pl.ds(pl.multiple_of(i * STRIP + j * ROWS, ROWS), ROWS)
            top = self.tops[rows, :]
            peak = jnp.max(top, axis=1, keepdims=True)
            total = jnp.sum(self.col[rows, :] * jnp.exp2(top - peak), axis=1, keepdims=True)
            out = peak + jnp.log(total) * LOG2E
            self.col[rows, :] = jnp.broadcast_to(out, (ROWS, 128))

    def partial(self, link, rows, tiles, first):
        source = self.alpha[self.time(link)]
        lanes = slice(tiles[0] * 128, tiles[-1] * 128 + 128)
        for low in range(rows.start, rows.stop, BAND):
            dots = jnp.dot(
                self.left[(link // 2) % 2][low:low + BAND, :],
                self.right[(link // 2) % 2][:, lanes],
                preferred_element_type=jnp.float32,
            )
            for j in range(0, BAND, ROWS):
                here = slice(low + j, low + j + ROWS)
                s = [
                    dots[j:j + ROWS, n * 128:n * 128 + 128] + source[:, c * 128:c * 128 + 128]
                    for n, c in enumerate(tiles)
                ]
                top = functools.reduce(jnp.maximum, s)
                if not first:
                    old = self.tops[here, :]
                    top = jnp.maximum(top, old)
                total = functools.reduce(jnp.add, [jnp.exp2(a - top) for a in s])
                if not first:
                    total = total + self.col[here, :] * jnp.exp2(old - top)
                self.tops[here, :] = top
                self.col[here, :] = total

    def message(self, link, i):
        after = self.time(link + 1)
        if link % 2 == 0:
            self.partial(link, slice(0, self.tiles * 128), range(self.tiles), True)
        else:
            lanes = pl.ds(pl.multiple_of(i * STRIP, STRIP), STRIP)
            cells = self.col.shape[0]
            step = BLOCK
            peak = total = None
            dots = jnp.dot(self.left[(link // 2) % 2][...], self.right[((link + 1) // 2) % 2][:, lanes], preferred_element_type=jnp.float32)
            for j in range(cells // step):
                rows = slice(j * step, (j + 1) * step)
                source = self.col[rows, :]
                s = dots[rows, :] + jnp.concatenate([source] * (STRIP // 128), axis=1)
                s = s.reshape(step // 8, 8, STRIP)
                top = jnp.max(s, axis=0)
                if peak is None:
                    peak = top
                    total = jnp.sum(jnp.exp2(s - peak[None]), axis=0)
                else:
                    new = jnp.maximum(peak, top)
                    total = total * jnp.exp2(peak - new) + jnp.sum(jnp.exp2(s - new[None]), axis=0)
                    peak = new
            top = jnp.max(peak, axis=0, keepdims=True)
            total = jnp.sum(total * jnp.exp2(peak - top), axis=0, keepdims=True)
            self.alpha[after, :, lanes] = self.const[after, :, lanes] + top + jnp.log(total) * LOG2E

    def keep(self, k):
        t = self.time(k)
        mine = pl.ds(pl.multiple_of(self.at * 128, 128), 128)
        if k % 2 == 0:
            self.own[t] = self.alpha[t, :, mine]
        else:
            block = self.col[mine, :]
            eye = lax.broadcasted_iota(jnp.int32, (128, 128), 0) == lax.broadcasted_iota(
                jnp.int32, (128, 128), 1
            )
            self.own[t] = jnp.sum(jnp.where(eye, block, 0.0), axis=0, keepdims=True)

    def log_total(self):
        phi = self.alpha[self.time(self.links)] + self.rest[...]
        peak = jnp.max(phi, axis=1, keepdims=True)
        return peak + jnp.log(jnp.sum(jnp.exp2(phi - peak), axis=1, keepdims=True)) * LOG2E

    def loop(self, count, body):
        def turn(i, carry):
            body(i)
            return carry

        lax.fori_loop(0, count, turn, 0)

    def whole(self, action, low=0, high=None):
        for r in range(low, self.tiles if high is None else high):
            action(r)

    def run(self, ready, done):
        half = self.links // 2
        line = self.tiles // 2
        near, far = slice(0, line * 128), slice(line * 128, self.tiles * 128)
        ready(0)
        self.whole(lambda r: self.constants(0, r), high=line)
        self.whole(lambda r: self.prep_even(0, r), high=line)
        self.whole(lambda r: self.constants(1, r), high=line)
        self.whole(lambda r: self.prep_odd(1, r), high=line)
        self.partial(0, near, range(line), True)
        ready("sources")
        self.whole(lambda r: self.constants(0, r), low=line)
        self.whole(lambda r: self.prep_even(0, r), low=line)
        self.partial(0, near, range(line, self.tiles), False)
        ready(1)
        self.whole(lambda r: self.constants(1, r), low=line)
        self.whole(lambda r: self.prep_odd(1, r), low=line)
        self.partial(0, far, range(self.tiles), True)
        for link in range(self.links):
            early = link + 1 < self.links and link >= half - 1
            if early:
                ready(link + 2)
            if link:
                self.message(link, 0)
            if early:
                self.whole(lambda r: self.prep(link + 1, r))
            if link % 2 == 0:
                self.reduce_lanes(0)
            self.keep(link + 1)
            done(link + 1)
            if link + 1 < self.links and not early:
                ready(link + 2)
                self.whole(lambda r: self.prep(link + 1, r))


def chain_kernel(links, tiles, pts, pot, out, *scratch):
    held, *pairs = scratch[:5]
    right, left = pairs[0:2], pairs[2:4]
    alpha, const, rest, col, own, other = scratch[5:11]
    block_send, line_recv, pair_recv, core_send, core_recv, end_send, end_recv = scratch[11:18]
    fill, tops, own_pts, own_pot, stage = scratch[18:]
    me = lax.axis_index("tile")
    way = lax.axis_index("link")
    line = tiles // 2
    at, side = me // 2, me % 2
    half = links // 2
    chunks = [(k, 1) for k in range(half + 1)]
    time = lambda k: k + way * (links - 2 * k)
    first = lambda k, count: k + way * (links - 2 * k - count + 1)
    slot = lambda z, y: 2 * z + y
    place = lambda r: slot(r % line, side if r < line else 1 - side)
    ahead = lambda d: slot(lax.rem(at + d, line), side)
    behind = lambda d: lax.rem(at + line - d, line)
    chain = Chain(
        links, tiles, pts.shape[1], held, right, left, alpha, const, rest, col, own, tops, at, place, time
    )

    early = pl.ds(way * half, half + 1)
    mine = [
        pltpu.make_async_copy(pot, own_pot, fill.at[0]),
        pltpu.make_async_copy(pts.at[early], own_pts, fill.at[1]),
    ]
    for copy in mine:
        copy.start()

    barrier = pltpu.get_barrier_semaphore()
    peers = [{"tile": ahead(d)} for d in range(1, line)]
    peers += [{"tile": slot(at, 1 - side)}, {"link": 1 - way}]
    for peer in peers:
        pl.semaphore_signal(barrier, inc=1, device_id=peer)
    for copy in mine:
        copy.wait()
    for j in range(half + 1):
        t = way * half + j
        block = jnp.concatenate([own_pts[j], own_pot[pl.ds(t, 1), :]], axis=0)
        stage[j] = block
        held[t, me] = block
    for buffer in right:
        buffer[192:256, :] = jnp.zeros((64, tiles * 128), jnp.bfloat16)
    pl.semaphore_wait(barrier, len(peers))

    def views(c, origin, source_own):
        k, count = chunks[c]
        span = pl.ds(first(k, count), count)
        part = pl.ds(first(k, count) - way * half, count)
        return (stage.at[part] if source_own else held.at[span, origin]), held.at[span, origin]

    def remote(c, origin, source_own, recv, device):
        src, dst = views(c, origin, source_own)
        return pltpu.make_async_remote_copy(
            src_ref=src,
            dst_ref=dst,
            send_sem=block_send.at[0],
            recv_sem=recv,
            device_id=device,
        )

    partner = {"tile": slot(at, 1 - side)}
    sent = []

    def all_of(span, send, recv, device):
        return pltpu.make_async_remote_copy(
            src_ref=span, dst_ref=span, send_sem=send, recv_sem=recv, device_id=device
        )

    def to_line(c, d):
        remote(c, me, True, line_recv.at[c, d - 1], {"tile": ahead(d)}).start()

    def to_pair(c, d):
        origin = slot(behind(d), side)
        remote(c, origin, d == 0, pair_recv.at[c], partner).start()

    def forward(c):
        for d in range(1, line):
            origin = slot(behind(d), side)
            remote(c, origin, False, line_recv.at[c, d - 1], partner).wait_recv()
            to_pair(c, d)

    def arrive(c):
        span = held.at[time(chunks[c][0]), pl.ds(0, line)]
        all_of(span, block_send.at[0], pair_recv.at[c], partner).wait_recv()

    def across(k):
        t = time(k)
        copy = pltpu.make_async_remote_copy(
            src_ref=held.at[t],
            dst_ref=held.at[t],
            send_sem=core_send.at[0],
            recv_sem=core_recv.at[0],
            device_id={"link": 1 - way},
        )
        copy.start()

    def from_core():
        blocks = held.at[pl.ds(0, half)]
        all_of(blocks, core_send.at[0], core_recv.at[0], {"link": 1 - way}).wait_recv()

    def rows(which):
        return pl.ds(first(half, half), half) if which == 0 else pl.ds(time(links), 1)

    def ends(which, span):
        return pltpu.make_async_remote_copy(
            src_ref=own.at[span],
            dst_ref=other.at[span],
            send_sem=end_send.at[which],
            recv_sem=end_recv.at[which],
            device_id={"link": 1 - way},
        )

    for c in range(len(chunks)):
        for d in range(line - 1, 0, -1):
            to_line(c, d)
        to_pair(c, 0)

    def ready(k):
        if k == 0:
            for c in range(3):
                forward(c)
        elif k == "sources":
            arrive(0)
            across(0)
        elif k <= half:
            if k + 2 <= half:
                forward(k + 2)
            arrive(k)
            if k < half:
                across(k)
        elif k == half + 1:
            from_core()

    def done(k):
        if k == links:
            for which in range(2):
                copy = ends(which, rows(which))
                copy.start()
                sent.append(copy)

    chain.run(ready, done)
    chain.keep(0)
    tops[0:1, :] = jnp.broadcast_to(chain.log_total(), (1, 128))
    lanes = pl.ds(pl.multiple_of(at * 128, 128), 128)
    for j in range(half):
        t = 1 + way * half + j
        tops[pl.ds(8 + j, 1), :] = own[t] - const[t, :, lanes]
    blocks = held.at[pl.ds(0, half + 1), pl.ds(0, 2 * line - 1)]
    all_of(blocks, block_send.at[0], pair_recv.at[0], partner).wait_send()
    all_of(held.at[pl.ds(0, half)], core_send.at[0], core_recv.at[0], {"link": 1 - way}).wait_send()
    ends(0, rows_other(0, links, half, way)).wait_recv()
    ends(1, rows_other(1, links, half, way)).wait_recv()
    keep = -math.log(tiles * 128)
    total = tops[0:1, :]
    for j in range(half):
        t = 1 + way * half + j
        combined = other[t] + tops[8 + j:9 + j, :]
        out[pl.ds(j, 1), :] = keep - (combined - total) / LOG2E
    for copy in sent:
        copy.wait_send()


def rows_other(which, links, half, way):
    back = 1 - way
    if which == 0:
        return pl.ds(half + back * (1 - half), half)
    return pl.ds(links - back * links, 1)


def local_fast(points, potentials):
    times, pcs, cell_dev = points.shape
    links = times - 1
    tiles = lax.axis_size("tile")
    cells = tiles * cell_dev
    vmem = pl.BlockSpec(memory_space=pltpu.VMEM)
    hbm = pl.BlockSpec(memory_space=pltpu.HBM)
    dma = pltpu.SemaphoreType.DMA
    phases = links // 2 + 1
    line = tiles // 2
    return pl.pallas_call(
        functools.partial(chain_kernel, links, tiles),
        out_shape=jax.ShapeDtypeStruct((links // 2, 128), jnp.float32),
        in_specs=[hbm] * 2,
        out_specs=vmem,
        scratch_shapes=[
            pltpu.VMEM((times, tiles, pcs + 1, 128), jnp.float32),
            pltpu.VMEM((256, cells), jnp.bfloat16),
            pltpu.VMEM((256, cells), jnp.bfloat16),
            pltpu.VMEM((cells, 256), jnp.bfloat16),
            pltpu.VMEM((cells, 256), jnp.bfloat16),
            pltpu.VMEM((times, 1, cells), jnp.float32),
            pltpu.VMEM((times, 1, cells), jnp.float32),
            pltpu.VMEM((1, cells), jnp.float32),
            pltpu.VMEM((cells, 128), jnp.float32),
            pltpu.VMEM((times, 1, 128), jnp.float32),
            pltpu.VMEM((times, 1, 128), jnp.float32),
            dma((1,)),
            dma((phases, line - 1)),
            dma((phases,)),
            dma((1,)),
            dma((1,)),
            dma((2,)),
            dma((2,)),
            dma((2,)),
            pltpu.VMEM((cells, 128), jnp.float32),
            pltpu.VMEM((links // 2 + 1, pcs, 128), jnp.float32),
            pltpu.VMEM((times, 128), jnp.float32),
            pltpu.VMEM((links // 2 + 1, pcs + 1, 128), jnp.float32),
        ],
        compiler_params=pltpu.CompilerParams(
            vmem_limit_bytes=66900000, collective_id=0, has_side_effects=True
        ),
    )(points, potentials)


def passed_along(block, axis, distance):
    devices = range(lax.axis_size(axis))
    route = [(i - distance, i) for i in devices if i - distance in devices]
    return lax.ppermute(block, axis, route)


def joined(part, axis, combine):
    gathered = jax.tree.map(lambda a: lax.all_gather(a, axis), part)

    def take(source):
        return jax.tree.map(lambda a: lax.dynamic_index_in_dim(a, source, 0, False), gathered)

    return lax.fori_loop(
        1, lax.axis_size(axis), lambda source, state: combine(state, take(source)), take(0)
    )


def pair_scores(source_pts, target_pts, source_msg):
    source_sq = jnp.sum(source_pts * source_pts, axis=0)
    target_sq = jnp.sum(target_pts * target_pts, axis=0)
    inner_prod = lax.dot_general(
        source_pts,
        target_pts,
        (((0,), (0,)), ((), ())),
        precision=lax.Precision.HIGHEST,
        preferred_element_type=jnp.float32,
    )
    pair_cost = source_sq[:, None] + target_sq[None, :] - 2.0 * inner_prod
    return source_msg[:, None] - pair_cost / EPSILON


def combine_lse(left_pair, right_pair):
    peak = jnp.maximum(left_pair[0], right_pair[0])
    return (
        peak,
        left_pair[1] * jnp.exp(left_pair[0] - peak) + right_pair[1] * jnp.exp(right_pair[0] - peak),
    )


def local(points, potentials):
    link_index = lax.axis_index("link")
    link_count = lax.axis_size("link")
    tile_count = lax.axis_size("tile")
    per_link = (points.shape[0] - 1) // link_count
    cell_dev = points.shape[2]
    total_cells = tile_count * cell_dev
    offset_link = link_index * per_link
    local_pts = lax.dynamic_slice_in_dim(points, offset_link, per_link + 1, 0)
    local_pot = lax.dynamic_slice_in_dim(potentials, offset_link, per_link + 1, 0)
    every_pts = lax.all_gather(local_pts, "tile", axis=2, tiled=True)

    def message(source_idx, target_idx, source_msg):
        source_pts = local_pts[source_idx]
        target_pot = local_pot[target_idx]
        target_all = every_pts[target_idx]
        scores = pair_scores(source_pts, target_all, source_msg)
        peak = jnp.max(scores, axis=0)
        partial_lse = peak + jnp.log(jnp.sum(jnp.exp(scores - peak[None, :]), axis=0))
        lse_parts = lax.all_to_all(
            partial_lse.reshape(tile_count, cell_dev),
            "tile",
            split_axis=0,
            concat_axis=0,
            tiled=True,
        )
        peak = jnp.max(lse_parts, axis=0)
        summed = jnp.sum(jnp.exp(lse_parts - peak[None, :]), axis=0)
        return target_pot + peak + jnp.log(summed)

    def sweep(start_msg, forward):
        start_pos = jnp.where(forward, 0, per_link).astype(jnp.int32)
        stored = jnp.zeros((per_link + 1, cell_dev), jnp.float32)
        stored = lax.dynamic_update_slice_in_dim(stored, start_msg[None, :], start_pos, 0)
        current = start_msg
        for link_step in range(per_link):
            source_idx = jnp.where(forward, link_step, per_link - link_step).astype(jnp.int32)
            target_idx = jnp.where(forward, link_step + 1, per_link - 1 - link_step).astype(
                jnp.int32
            )
            current = message(source_idx, target_idx, current)
            stored = lax.dynamic_update_slice_in_dim(stored, current[None, :], target_idx, 0)
        return stored

    first_end = link_index == 0
    early_pass = sweep(local_pot[0], True)
    handed = passed_along(early_pass[per_link], "link", 1)
    forward_msgs = sweep(jnp.where(first_end, local_pot[0], handed), True)
    late_pass = sweep(local_pot[per_link], False)
    handed_back = passed_along(late_pass[0], "link", -1)
    backward_msgs = sweep(jnp.where(first_end, handed_back, local_pot[per_link]), False)
    combined = forward_msgs + backward_msgs - local_pot
    last_row = combined[per_link]
    peak = jnp.max(last_row)
    summed = jnp.sum(jnp.exp(last_row - peak))
    peak, summed = joined((peak, summed), "tile", combine_lse)
    log_total = peak + jnp.log(summed)
    return -math.log(total_cells) - (combined[1:] - log_total)


def fits(mesh, points):
    times, pcs, total = points.shape
    cell_dev = total // (mesh.shape["groups"] * mesh.shape["tile"])
    cells = cell_dev * mesh.shape["tile"]
    held = 2 * cells * cells * 4 + 2 * times * cells * 32 * 4
    return (
        cell_dev == 128
        and pcs < 31
        and times % 2 == 1
        and mesh.shape["tile"] % 2 == 0
        and cells % STRIP == 0
        and mesh.shape["link"] == 2
        and held < 32 * 1024 * 1024
    )


def solution(mesh):
    placed = (P(None, None, ("groups", "tile")), P(None, ("groups", "tile")))

    def whole(points, potentials):
        body = local_fast if fits(mesh, points) else local
        return jax.shard_map(
            body, mesh=mesh, in_specs=placed, out_specs=P("link", ("groups", "tile")), check_vma=False
        )(points, potentials)

    return whole
```

```python
import functools
import math

import jax
import jax.numpy as jnp
from jax import lax
from jax.experimental import pallas as pl
from jax.experimental.pallas import tpu as pltpu
from jax.sharding import PartitionSpec as P

EPSILON = 0.5
LOG2E = math.log2(math.e)
SCALE = 2.0 / EPSILON * LOG2E
STRIP = 1024
ROWS = 8
BLOCK = 32
BAND = 512


def pieces(value):
    high = value.astype(jnp.bfloat16)
    rest = value - high.astype(jnp.float32)
    middle = rest.astype(jnp.bfloat16)
    low = (rest - middle.astype(jnp.float32)).astype(jnp.bfloat16)
    return high, middle, low


def padded(points, extra, slot):
    pad = 32 - points.shape[0]
    row = lax.broadcasted_iota(jnp.int32, (pad, points.shape[1]), 0)
    tail = jnp.where(row == slot, extra, 0.0)
    return jnp.concatenate([points, tail], axis=0)


class Chain:
    def __init__(self, links, tiles, pcs, pts, right, left, alpha, const, rest, col, own, tops, at, place, time):
        self.links, self.tiles = links, tiles
        self.pts, self.pcs = pts, pcs
        self.right, self.left = right, left
        self.alpha, self.const, self.rest = alpha, const, rest
        self.col, self.own, self.tops = col, own, tops
        self.at, self.place, self.time = at, place, time

    def constants(self, k, r):
        t = self.time(k)
        x = self.pts[t, self.place(r), : self.pcs]
        lanes = pl.ds(pl.multiple_of(r * 128, 128), 128)
        square = jnp.sum(x * x, axis=0, keepdims=True)
        pot = self.pts[t, self.place(r), self.pcs :]
        self.const[t, :, lanes] = (pot - (2.0 / EPSILON) * square) * LOG2E
        if k == 0:
            self.alpha[t, :, lanes] = (pot - square / EPSILON) * LOG2E
        if k == self.links:
            self.rest[:, lanes] = square * (LOG2E / EPSILON)

    def prep_even(self, k, r):
        slot = (k // 2) % 2
        x = self.pts[self.time(k), self.place(r), : self.pcs]
        h, m, l = pieces(padded(x, jnp.ones((1, 128), jnp.float32), slot))
        lanes = pl.ds(pl.multiple_of(r * 128, 128), 128)
        self.right[slot][0:192, lanes] = jnp.concatenate([h, h, h, m, l, m], axis=0)

    def prep_odd(self, k, r):
        slot = (k // 2) % 2
        t = self.time(k)
        lanes = pl.ds(pl.multiple_of(r * 128, 128), 128)
        x = self.pts[t, self.place(r), : self.pcs] * SCALE
        h, m, l = pieces(padded(x, self.const[t, :, lanes], slot))
        block = jnp.concatenate([h, m, l, h], axis=0)
        block = block.T
        self.left[slot][lanes, 0:128] = block
        self.left[slot][lanes, 128:256] = block

    def prep(self, link, r):
        self.constants(link + 1, r)
        if link % 2 == 0:
            self.prep_odd(link + 1, r)
        else:
            self.prep_even(link + 1, r)

    def reduce_lanes(self, i):
        for j in range(STRIP // ROWS):
            rows = pl.ds(pl.multiple_of(i * STRIP + j * ROWS, ROWS), ROWS)
            top = self.tops[rows, :]
            peak = jnp.max(top, axis=1, keepdims=True)
            total = jnp.sum(self.col[rows, :] * jnp.exp2(top - peak), axis=1, keepdims=True)
            out = peak + jnp.log(total) * LOG2E
            self.col[rows, :] = jnp.broadcast_to(out, (ROWS, 128))

    def partial(self, link, rows, tiles, first):
        source = self.alpha[self.time(link)]
        lanes = slice(tiles[0] * 128, tiles[-1] * 128 + 128)
        for low in range(rows.start, rows.stop, BAND):
            dots = jnp.dot(
                self.left[(link // 2) % 2][low:low + BAND, :],
                self.right[(link // 2) % 2][:, lanes],
                preferred_element_type=jnp.float32,
            )
            for j in range(0, BAND, ROWS):
                here = slice(low + j, low + j + ROWS)
                s = [
                    dots[j:j + ROWS, n * 128:n * 128 + 128] + source[:, c * 128:c * 128 + 128]
                    for n, c in enumerate(tiles)
                ]
                top = functools.reduce(jnp.maximum, s)
                if not first:
                    old = self.tops[here, :]
                    top = jnp.maximum(top, old)
                total = functools.reduce(jnp.add, [jnp.exp2(a - top) for a in s])
                if not first:
                    total = total + self.col[here, :] * jnp.exp2(old - top)
                self.tops[here, :] = top
                self.col[here, :] = total

    def message(self, link, i):
        after = self.time(link + 1)
        if link % 2 == 0:
            self.partial(link, slice(0, self.tiles * 128), range(self.tiles), True)
        else:
            lanes = pl.ds(pl.multiple_of(i * STRIP, STRIP), STRIP)
            cells = self.col.shape[0]
            step = BLOCK
            peak = total = None
            dots = jnp.dot(self.left[(link // 2) % 2][...], self.right[((link + 1) // 2) % 2][:, lanes], preferred_element_type=jnp.float32)
            for j in range(cells // step):
                rows = slice(j * step, (j + 1) * step)
                source = self.col[rows, :]
                s = dots[rows, :] + jnp.concatenate([source] * (STRIP // 128), axis=1)
                s = s.reshape(step // 8, 8, STRIP)
                top = jnp.max(s, axis=0)
                if peak is None:
                    peak = top
                    total = jnp.sum(jnp.exp2(s - peak[None]), axis=0)
                else:
                    new = jnp.maximum(peak, top)
                    total = total * jnp.exp2(peak - new) + jnp.sum(jnp.exp2(s - new[None]), axis=0)
                    peak = new
            top = jnp.max(peak, axis=0, keepdims=True)
            total = jnp.sum(total * jnp.exp2(peak - top), axis=0, keepdims=True)
            self.alpha[after, :, lanes] = self.const[after, :, lanes] + top + jnp.log(total) * LOG2E

    def keep(self, k):
        t = self.time(k)
        mine = pl.ds(pl.multiple_of(self.at * 128, 128), 128)
        if k % 2 == 0:
            self.own[t] = self.alpha[t, :, mine]
        else:
            block = self.col[mine, :]
            eye = lax.broadcasted_iota(jnp.int32, (128, 128), 0) == lax.broadcasted_iota(
                jnp.int32, (128, 128), 1
            )
            self.own[t] = jnp.sum(jnp.where(eye, block, 0.0), axis=0, keepdims=True)

    def log_total(self):
        phi = self.alpha[self.time(self.links)] + self.rest[...]
        peak = jnp.max(phi, axis=1, keepdims=True)
        return peak + jnp.log(jnp.sum(jnp.exp2(phi - peak), axis=1, keepdims=True)) * LOG2E

    def loop(self, count, body):
        def turn(i, carry):
            body(i)
            return carry

        lax.fori_loop(0, count, turn, 0)

    def whole(self, action, low=0, high=None):
        for r in range(low, self.tiles if high is None else high):
            action(r)

    def run(self, ready, done):
        half = self.links // 2
        line = self.tiles // 2
        near, far = slice(0, line * 128), slice(line * 128, self.tiles * 128)
        ready(0)
        self.whole(lambda r: self.constants(0, r), high=line)
        self.whole(lambda r: self.prep_even(0, r), high=line)
        self.whole(lambda r: self.constants(1, r), high=line)
        self.whole(lambda r: self.prep_odd(1, r), high=line)
        self.partial(0, near, range(line), True)
        ready("sources")
        self.whole(lambda r: self.constants(0, r), low=line)
        self.whole(lambda r: self.prep_even(0, r), low=line)
        self.partial(0, near, range(line, self.tiles), False)
        ready(1)
        self.whole(lambda r: self.constants(1, r), low=line)
        self.whole(lambda r: self.prep_odd(1, r), low=line)
        self.partial(0, far, range(self.tiles), True)
        for link in range(self.links):
            early = link + 1 < self.links and link >= half - 1
            if early:
                ready(link + 2)
            if link:
                self.message(link, 0)
            if early:
                self.whole(lambda r: self.prep(link + 1, r))
            if link % 2 == 0:
                self.reduce_lanes(0)
            self.keep(link + 1)
            done(link + 1)
            if link + 1 < self.links and not early:
                ready(link + 2)
                self.whole(lambda r: self.prep(link + 1, r))


def chain_kernel(links, tiles, pts, pot, out, *scratch):
    held, *pairs = scratch[:5]
    right, left = pairs[0:2], pairs[2:4]
    alpha, const, rest, col, own, other = scratch[5:11]
    block_send, line_recv, pair_recv, core_send, core_recv, end_send, end_recv = scratch[11:18]
    fill, tops, own_pts, own_pot, stage = scratch[18:]
    me = lax.axis_index("tile")
    way = lax.axis_index("link")
    line = tiles // 2
    at, side = me // 2, me % 2
    half = links // 2
    chunks = [(k, 1) for k in range(half + 1)]
    time = lambda k: k + way * (links - 2 * k)
    first = lambda k, count: k + way * (links - 2 * k - count + 1)
    slot = lambda z, y: 2 * z + y
    place = lambda r: slot(r % line, side if r < line else 1 - side)
    ahead = lambda d: slot(lax.rem(at + d, line), side)
    behind = lambda d: lax.rem(at + line - d, line)
    chain = Chain(
        links, tiles, pts.shape[1], held, right, left, alpha, const, rest, col, own, tops, at, place, time
    )

    early = pl.ds(way * half, half + 1)
    mine = [
        pltpu.make_async_copy(pot, own_pot, fill.at[0]),
        pltpu.make_async_copy(pts.at[early], own_pts, fill.at[1]),
    ]
    for copy in mine:
        copy.start()

    barrier = pltpu.get_barrier_semaphore()
    peers = [{"tile": ahead(d)} for d in range(1, line)]
    peers += [{"tile": slot(at, 1 - side)}, {"link": 1 - way}]
    for peer in peers:
        pl.semaphore_signal(barrier, inc=1, device_id=peer)
    for copy in mine:
        copy.wait()
    for j in range(half + 1):
        t = way * half + j
        block = jnp.concatenate([own_pts[j], own_pot[pl.ds(t, 1), :]], axis=0)
        stage[j] = block
        held[t, me] = block
    for buffer in right:
        buffer[192:256, :] = jnp.zeros((64, tiles * 128), jnp.bfloat16)
    pl.semaphore_wait(barrier, len(peers))

    def views(c, origin, source_own):
        k, count = chunks[c]
        span = pl.ds(first(k, count), count)
        part = pl.ds(first(k, count) - way * half, count)
        return (stage.at[part] if source_own else held.at[span, origin]), held.at[span, origin]

    def remote(c, origin, source_own, recv, device):
        src, dst = views(c, origin, source_own)
        return pltpu.make_async_remote_copy(
            src_ref=src,
            dst_ref=dst,
            send_sem=block_send.at[0],
            recv_sem=recv,
            device_id=device,
        )

    partner = {"tile": slot(at, 1 - side)}
    sent = []

    def all_of(span, send, recv, device):
        return pltpu.make_async_remote_copy(
            src_ref=span, dst_ref=span, send_sem=send, recv_sem=recv, device_id=device
        )

    def to_line(c, d):
        remote(c, me, True, line_recv.at[c, d - 1], {"tile": ahead(d)}).start()

    def to_pair(c, d):
        origin = slot(behind(d), side)
        remote(c, origin, d == 0, pair_recv.at[c], partner).start()

    def forward(c):
        for d in range(1, line):
            origin = slot(behind(d), side)
            remote(c, origin, False, line_recv.at[c, d - 1], partner).wait_recv()
            to_pair(c, d)

    def arrive(c):
        span = held.at[time(chunks[c][0]), pl.ds(0, line)]
        all_of(span, block_send.at[0], pair_recv.at[c], partner).wait_recv()

    def across(k):
        t = time(k)
        copy = pltpu.make_async_remote_copy(
            src_ref=held.at[t],
            dst_ref=held.at[t],
            send_sem=core_send.at[0],
            recv_sem=core_recv.at[0],
            device_id={"link": 1 - way},
        )
        copy.start()

    def from_core():
        blocks = held.at[pl.ds(0, half)]
        all_of(blocks, core_send.at[0], core_recv.at[0], {"link": 1 - way}).wait_recv()

    def rows(which):
        return pl.ds(first(half, half), half) if which == 0 else pl.ds(time(links), 1)

    def ends(which, span):
        return pltpu.make_async_remote_copy(
            src_ref=own.at[span],
            dst_ref=other.at[span],
            send_sem=end_send.at[0],
            recv_sem=end_recv.at[0],
            device_id={"link": 1 - way},
        )

    for c in range(len(chunks)):
        for d in range(line - 1, 0, -1):
            to_line(c, d)
        to_pair(c, 0)

    def ready(k):
        if k == 0:
            for c in range(3):
                forward(c)
        elif k == "sources":
            arrive(0)
            across(0)
        elif k <= half:
            if k + 2 <= half:
                forward(k + 2)
            arrive(k)
            if k < half:
                across(k)
        elif k == half + 1:
            from_core()

    def done(k):
        if k == links:
            for which in range(2):
                copy = ends(which, rows(which))
                copy.start()
                sent.append(copy)

    chain.run(ready, done)
    chain.keep(0)
    tops[0:1, :] = jnp.broadcast_to(chain.log_total(), (1, 128))
    lanes = pl.ds(pl.multiple_of(at * 128, 128), 128)
    for j in range(half):
        t = 1 + way * half + j
        tops[pl.ds(8 + j, 1), :] = own[t] - const[t, :, lanes]
    blocks = held.at[pl.ds(0, half + 1), pl.ds(0, 2 * line - 1)]
    all_of(blocks, block_send.at[0], pair_recv.at[0], partner).wait_send()
    all_of(held.at[pl.ds(0, half)], core_send.at[0], core_recv.at[0], {"link": 1 - way}).wait_send()
    rest_of = ends(0, pl.ds(0, half + 1))
    rest_of.wait_recv()
    keep = -math.log(tiles * 128)
    total = tops[0:1, :]
    for j in range(half):
        t = 1 + way * half + j
        combined = other[t] + tops[8 + j:9 + j, :]
        out[pl.ds(j, 1), :] = keep - (combined - total) / LOG2E
    rest_of.wait_send()


def rows_other(which, links, half, way):
    back = 1 - way
    if which == 0:
        return pl.ds(half + back * (1 - half), half)
    return pl.ds(links - back * links, 1)


def local_fast(points, potentials):
    times, pcs, cell_dev = points.shape
    links = times - 1
    tiles = lax.axis_size("tile")
    cells = tiles * cell_dev
    vmem = pl.BlockSpec(memory_space=pltpu.VMEM)
    hbm = pl.BlockSpec(memory_space=pltpu.HBM)
    dma = pltpu.SemaphoreType.DMA
    phases = links // 2 + 1
    line = tiles // 2
    return pl.pallas_call(
        functools.partial(chain_kernel, links, tiles),
        out_shape=jax.ShapeDtypeStruct((links // 2, 128), jnp.float32),
        in_specs=[hbm] * 2,
        out_specs=vmem,
        scratch_shapes=[
            pltpu.VMEM((times, tiles, pcs + 1, 128), jnp.float32),
            pltpu.VMEM((256, cells), jnp.bfloat16),
            pltpu.VMEM((256, cells), jnp.bfloat16),
            pltpu.VMEM((cells, 256), jnp.bfloat16),
            pltpu.VMEM((cells, 256), jnp.bfloat16),
            pltpu.VMEM((times, 1, cells), jnp.float32),
            pltpu.VMEM((times, 1, cells), jnp.float32),
            pltpu.VMEM((1, cells), jnp.float32),
            pltpu.VMEM((cells, 128), jnp.float32),
            pltpu.VMEM((times, 1, 128), jnp.float32),
            pltpu.VMEM((times, 1, 128), jnp.float32),
            dma((1,)),
            dma((phases, line - 1)),
            dma((phases,)),
            dma((1,)),
            dma((1,)),
            dma((1,)),
            dma((1,)),
            dma((2,)),
            pltpu.VMEM((cells, 128), jnp.float32),
            pltpu.VMEM((links // 2 + 1, pcs, 128), jnp.float32),
            pltpu.VMEM((times, 128), jnp.float32),
            pltpu.VMEM((links // 2 + 1, pcs + 1, 128), jnp.float32),
        ],
        compiler_params=pltpu.CompilerParams(
            vmem_limit_bytes=66900000, collective_id=0, has_side_effects=True
        ),
    )(points, potentials)


def passed_along(block, axis, distance):
    devices = range(lax.axis_size(axis))
    route = [(i - distance, i) for i in devices if i - distance in devices]
    return lax.ppermute(block, axis, route)


def joined(part, axis, combine):
    gathered = jax.tree.map(lambda a: lax.all_gather(a, axis), part)

    def take(source):
        return jax.tree.map(lambda a: lax.dynamic_index_in_dim(a, source, 0, False), gathered)

    return lax.fori_loop(
        1, lax.axis_size(axis), lambda source, state: combine(state, take(source)), take(0)
    )


def pair_scores(source_pts, target_pts, source_msg):
    source_sq = jnp.sum(source_pts * source_pts, axis=0)
    target_sq = jnp.sum(target_pts * target_pts, axis=0)
    inner_prod = lax.dot_general(
        source_pts,
        target_pts,
        (((0,), (0,)), ((), ())),
        precision=lax.Precision.HIGHEST,
        preferred_element_type=jnp.float32,
    )
    pair_cost = source_sq[:, None] + target_sq[None, :] - 2.0 * inner_prod
    return source_msg[:, None] - pair_cost / EPSILON


def combine_lse(left_pair, right_pair):
    peak = jnp.maximum(left_pair[0], right_pair[0])
    return (
        peak,
        left_pair[1] * jnp.exp(left_pair[0] - peak) + right_pair[1] * jnp.exp(right_pair[0] - peak),
    )


def local(points, potentials):
    link_index = lax.axis_index("link")
    link_count = lax.axis_size("link")
    tile_count = lax.axis_size("tile")
    per_link = (points.shape[0] - 1) // link_count
    cell_dev = points.shape[2]
    total_cells = tile_count * cell_dev
    offset_link = link_index * per_link
    local_pts = lax.dynamic_slice_in_dim(points, offset_link, per_link + 1, 0)
    local_pot = lax.dynamic_slice_in_dim(potentials, offset_link, per_link + 1, 0)
    every_pts = lax.all_gather(local_pts, "tile", axis=2, tiled=True)

    def message(source_idx, target_idx, source_msg):
        source_pts = local_pts[source_idx]
        target_pot = local_pot[target_idx]
        target_all = every_pts[target_idx]
        scores = pair_scores(source_pts, target_all, source_msg)
        peak = jnp.max(scores, axis=0)
        partial_lse = peak + jnp.log(jnp.sum(jnp.exp(scores - peak[None, :]), axis=0))
        lse_parts = lax.all_to_all(
            partial_lse.reshape(tile_count, cell_dev),
            "tile",
            split_axis=0,
            concat_axis=0,
            tiled=True,
        )
        peak = jnp.max(lse_parts, axis=0)
        summed = jnp.sum(jnp.exp(lse_parts - peak[None, :]), axis=0)
        return target_pot + peak + jnp.log(summed)

    def sweep(start_msg, forward):
        start_pos = jnp.where(forward, 0, per_link).astype(jnp.int32)
        stored = jnp.zeros((per_link + 1, cell_dev), jnp.float32)
        stored = lax.dynamic_update_slice_in_dim(stored, start_msg[None, :], start_pos, 0)
        current = start_msg
        for link_step in range(per_link):
            source_idx = jnp.where(forward, link_step, per_link - link_step).astype(jnp.int32)
            target_idx = jnp.where(forward, link_step + 1, per_link - 1 - link_step).astype(
                jnp.int32
            )
            current = message(source_idx, target_idx, current)
            stored = lax.dynamic_update_slice_in_dim(stored, current[None, :], target_idx, 0)
        return stored

    first_end = link_index == 0
    early_pass = sweep(local_pot[0], True)
    handed = passed_along(early_pass[per_link], "link", 1)
    forward_msgs = sweep(jnp.where(first_end, local_pot[0], handed), True)
    late_pass = sweep(local_pot[per_link], False)
    handed_back = passed_along(late_pass[0], "link", -1)
    backward_msgs = sweep(jnp.where(first_end, handed_back, local_pot[per_link]), False)
    combined = forward_msgs + backward_msgs - local_pot
    last_row = combined[per_link]
    peak = jnp.max(last_row)
    summed = jnp.sum(jnp.exp(last_row - peak))
    peak, summed = joined((peak, summed), "tile", combine_lse)
    log_total = peak + jnp.log(summed)
    return -math.log(total_cells) - (combined[1:] - log_total)


def fits(mesh, points):
    times, pcs, total = points.shape
    cell_dev = total // (mesh.shape["groups"] * mesh.shape["tile"])
    cells = cell_dev * mesh.shape["tile"]
    held = 2 * cells * cells * 4 + 2 * times * cells * 32 * 4
    return (
        cell_dev == 128
        and pcs < 31
        and times % 2 == 1
        and mesh.shape["tile"] % 2 == 0
        and cells % STRIP == 0
        and mesh.shape["link"] == 2
        and held < 32 * 1024 * 1024
    )


def solution(mesh):
    placed = (P(None, None, ("groups", "tile")), P(None, ("groups", "tile")))

    def whole(points, potentials):
        body = local_fast if fits(mesh, points) else local
        return jax.shard_map(
            body, mesh=mesh, in_specs=placed, out_specs=P("link", ("groups", "tile")), check_vma=False
        )(points, potentials)

    return whole
```
